256 devices in a mesh: rows: 128 (over x, z, y), cols: 2 (over core).
Axes of the slice: x: 4, y: 4, z: 8, core: 2. Of those that a mesh axis runs over, the one named last changes fastest.
Arguments:
- points: float32 [8, 32768], P(None, ('cols', 'rows')), may hold values from -6 to 6
- targets: float32 [32768], P(('cols', 'rows')), may hold values from -6 to 6
- noise: float32 [64, 32768], P(None, ('cols', 'rows')), may hold values from -6 to 6
- omega: float32 [8, 2048], P(None, 'rows'), may hold values from -12 to 12
- phase: float32 [2048], P('rows'), may hold values from -3.140625 to 3.140625
- weights: float32 [2048, 64], P('rows'), may hold values from -6 to 6
Outputs:
- posterior: float32 [64, 32768], P(None, ('cols', 'rows'))
- residual: float32 [64, 32768], P(None, ('cols', 'rows'))
The draws below stay inside these ranges and needn't reach their ends.
All inputs are finite; a program needn't handle non-finite values.
Results may differ from the reference program's by a relative error of at most 0.02.
Values may be sent and summed in bfloat16 or wider, within the bound.
A program may use at most 64 MiB of HBM per device.

```python
import math
import jax
import jax.numpy as jnp
from jax import lax

D_IN = 8
F = 2048
S = 64
ITERS = 2
N = 32768


def block_levels(own_key, extent, shards, least, high):
    def one(axis_at, blocks):
        draws = jax.random.uniform(jax.random.fold_in(jax.random.fold_in(own_key, 6), axis_at), (blocks,), jnp.float32, least / len(shards), high / len(shards))
        return jnp.repeat(jnp.exp(draws), extent[axis_at] // blocks).reshape((-1,) + (1,) * (len(extent) - axis_at - 1))

    gain = one(*shards[0])
    for cut in shards[1:]:
        gain = gain * one(*cut)
    return gain


def centred(stream_key, dims, spread, most, shards=(), held_as=jnp.bfloat16):
    factor_of = block_levels(stream_key, dims, shards, -0.22, 0.18) if shards else 1.0
    drawn = jax.random.normal(stream_key, dims, jnp.float32) * spread * factor_of
    return jnp.minimum(jnp.maximum(drawn, -most), most).astype(held_as)


def setup_inputs(seed: int = 0) -> dict:
    arg_keys = jax.random.split(jax.random.key(seed), 7)
    return {
        "points": centred(arg_keys[0], (D_IN, N), 1.0, 6.0, ((1, 256),), jnp.float32),
        "targets": centred(arg_keys[1], (N,), 1.0, 6.0, ((0, 256),), jnp.float32),
        "noise": centred(arg_keys[2], (S, N), 1.0, 6.0, ((1, 256),), jnp.float32),
        "omega": centred(arg_keys[3], (D_IN, F), 2.0, 12.0, ((1, 128),), jnp.float32),
        "phase": jnp.clip(jax.random.uniform(arg_keys[4], (F,), jnp.float32, -3.140625, 3.140625), -3.140625, 3.140625),
        "weights": centred(arg_keys[5], (F, S), 1.0, 6.0, ((0, 128),), jnp.float32),
    }


def kernel_block(left, right):
    cross = lax.dot_general(left, right, (((0,), (0,)), ((), ())), precision=lax.Precision.HIGHEST, preferred_element_type=jnp.float32)
    left_sq = lax.optimization_barrier(jnp.sum(left * left, 0))
    right_sq = lax.optimization_barrier(jnp.sum(right * right, 0))
    dist = left_sq[:, None] + right_sq[None, :] - 2.0 * cross
    return jnp.exp(-2.0 * dist).astype(jnp.bfloat16)

def apply_kernel(points, direction):
    width = math.gcd(N, 512)
    count = N // width
    low = direction.astype(jnp.bfloat16)
    blocks = points.reshape(D_IN, count, width).transpose(1, 0, 2)

    def one_block(block):
        return jnp.dot(low, kernel_block(points, block), preferred_element_type=jnp.float32)
    out = lax.map(one_block, blocks)
    return out.transpose(1, 0, 2).reshape(S, N)

def reference(points, targets, noise, omega, phase, weights):
    features = jnp.cos(jnp.dot(omega.T, points, precision=lax.Precision.HIGHEST, preferred_element_type=jnp.float32) + phase[:, None])
    prior = math.sqrt(2.0 / F) * jnp.dot(weights.T, features, precision=lax.Precision.HIGHEST, preferred_element_type=jnp.float32)
    rhs = targets[None, :] - prior - 0.5 * noise
    residual = rhs
    direction = rhs
    posterior = prior
    norm_now = lax.optimization_barrier(jnp.sum(residual * residual, 1))
    for step in range(ITERS):
        kernel_part = apply_kernel(points, direction)
        image = kernel_part + 0.25 * direction
        alpha = norm_now / lax.optimization_barrier(jnp.sum(direction * image, 1))
        posterior = posterior + alpha[:, None] * kernel_part
        residual = residual - alpha[:, None] * image
        if step + 1 < ITERS:
            norm_next = lax.optimization_barrier(jnp.sum(residual * residual, 1))
            direction = residual + (norm_next / norm_now)[:, None] * direction
            norm_now = norm_next
    return (posterior, residual)
```

```python
import functools
import math

import jax
import jax.numpy as jnp
from jax import lax
from jax.experimental import pallas as pl
from jax.experimental.pallas import tpu as pltpu
from jax.sharding import Mesh
from jax.sharding import PartitionSpec as P

AXES = ("px", "pz", "py", "cols")
ROWS = ("px", "pz", "py")
COLS_ROWS = ("cols", "px", "pz", "py")
MESH = pl.DeviceIdType.MESH
F32, BF16 = jnp.float32, jnp.bfloat16

D = 8
S = 64
B = 128
FB = 16
JITTER = 0.25
SPREAD = math.sqrt(4.0 * math.log2(math.e))
SINE = [(-1) ** k * (2.0 * math.pi) ** (2 * k + 1) / math.factorial(2 * k + 1) for k in range(6)]


def SLOTS(nz, np_):
    table = [("prm_z", nz), ("prm_p", np_), ("pts_z", nz), ("pts_p", np_), ("pts_d", np_), ("prior", 1)]
    for n in "01":
        table += [("low%s_p" % n, np_), ("low%s_d" % n, np_), ("low%s_z" % n, nz), ("out%s" % n, nz)]
    for name in ("cur0", "cur1", "mom"):
        table += [(name + "_z", 2 * nz), (name + "_p", np_)]
    return table


def three_parts(a):
    one = a.astype(BF16).astype(F32)
    rest = a - one
    two = rest.astype(BF16).astype(F32)
    three = (rest - two).astype(BF16).astype(F32)
    return one, two, three


def rows_of(pieces, width):
    row = lax.broadcasted_iota(jnp.int32, (8, width), 0)
    out = jnp.zeros((8, width), F32)
    for k, piece in enumerate(pieces):
        out = jnp.where(row == k, piece, out)
    return out


def exponent_left(points):
    scaled = points * SPREAD
    a1, a2, a3 = three_parts(scaled)
    n1, n2, n3 = three_parts(-0.5 * jnp.sum(scaled * scaled, 0, keepdims=True))
    width = points.shape[1]
    norms = rows_of((n1, n2, n3, 1.0, 1.0, 1.0), width)
    return jnp.concatenate([a1, a1, a2, a2, a1, a3, norms, jnp.zeros((8, width), F32)], 0)


def exponent_right(points):
    scaled = points * SPREAD
    b1, b2, b3 = three_parts(scaled)
    n1, n2, n3 = three_parts(-0.5 * jnp.sum(scaled * scaled, 0, keepdims=True))
    width = points.shape[1]
    norms = rows_of((1.0, 1.0, 1.0, n1, n2, n3), width)
    return jnp.concatenate([b1, b2, b1, b2, b3, b1, norms, jnp.zeros((8, width), F32)], 0)


def cos_turns(t):
    r = t - jnp.floor(t + 0.5)
    v = 0.25 - jnp.abs(r)
    w = v * v
    acc = jnp.full_like(w, SINE[-1])
    for c in SINE[-2::-1]:
        acc = acc * w + c
    return acc * v


def mm(a, b, dims=(((1,), (0,)), ((), ()))):
    return lax.dot_general(a, b, dims, preferred_element_type=F32)


def kernel(
    sizes,
    pts_ref, tgt_ref, noise_ref, prm_ref,
    post_ref, res_ref,
    prm, ptsj, ptsi, pside, prior_s, acc, rhs_s, low, low_z, right, kern, outb, rcv,
    mom_z, mom_p, cur_z, cur_p, send, recv,
):
    nx, nz, ny = sizes
    np_, half = nx * ny, nz // 2
    nfeat = nx * nz * ny * FB
    x, z, y, c = (lax.axis_index(a) for a in AXES)
    p = x * ny + y
    oc = 1 - c
    twin = (x, z, y, oc)

    at = {}
    top = 0
    for name, count in SLOTS(nz, np_):
        at[name] = top
        top += count

    def rdma(name, k, src, dst, dev):
        i = at[name] + k
        return pltpu.make_async_remote_copy(
            src_ref=src, dst_ref=dst, send_sem=send.at[i], recv_sem=recv.at[i],
            device_id=dev, device_id_type=MESH)

    def plane(d, sign=1):
        dx, dy = lax.div(d, ny), lax.rem(d, ny)
        if sign < 0:
            dx, dy = nx - dx, ny - dy
        return lax.rem(x + dx, nx), lax.rem(y + dy, ny)

    def plane_dev(d):
        xx, yy = plane(d)
        return (xx, z, yy, c)

    def plane_slot(d):
        xx, yy = plane(d, -1)
        return xx * ny + yy

    def zdev(d, core):
        return (x, lax.rem(z + d, nz), y, core)

    def zfrom(d):
        return lax.rem(z + nz - d, nz)

    def loop(lo, hi, f):
        def step(i, carry):
            f(i)
            return carry
        lax.fori_loop(lo, hi, step, 0)

    bar = pltpu.get_barrier_semaphore()

    def greet(dev):
        pl.semaphore_signal(bar, inc=1, device_id=dev, device_id_type=MESH)

    greet(twin)
    loop(1, nz, lambda d: greet(zdev(d, c)))
    loop(1, nz, lambda d: greet(zdev(d, oc)))
    loop(1, np_, lambda d: greet(plane_dev(d)))
    pl.semaphore_wait(bar, 1 + 2 * (nz - 1) + np_ - 1)

    mine = lax.rem(z, 2) == c
    zslot = lax.div(z, 2)

    @pl.when(mine)
    def _():
        loop(1, nz, lambda d: rdma("prm_z", d, prm_ref, prm.at[p, zslot], zdev(d, c)).start())
        prm[p, zslot] = prm_ref[...]

    rdma("pts_d", 0, pts_ref, ptsj.at[c * np_ + p], twin).start()
    loop(1, np_, lambda d: rdma("pts_p", d, pts_ref, ptsj.at[c * np_ + p], plane_dev(d)).start())
    loop(1, nz, lambda d: rdma("pts_z", d, pts_ref, ptsi.at[z], zdev(d, c)).start())
    ptsj[c * np_ + p] = pts_ref[...]
    ptsi[z] = pts_ref[...]

    def got(name, k, dst):
        rdma(name, k, dst, dst, twin).wait_recv()

    def prm_wait(k):
        d = 2 * k
        src = zfrom(d)
        got("prm_z", d, prm.at[p, lax.div(src, 2)])

    def prm_wait_odd(k):
        d = 2 * k + 1
        src = zfrom(d)
        got("prm_z", d, prm.at[p, lax.div(src, 2)])

    @pl.when(mine)
    def _():
        loop(1, half, prm_wait)

    @pl.when(jnp.logical_not(mine))
    def _():
        loop(0, half, prm_wait_odd)

    loop(1, np_, lambda d: rdma("prm_p", d, prm.at[p], prm.at[p], plane_dev(d)).start())

    def pts_forward(d):
        slot = ptsj.at[c * np_ + plane_slot(d)]
        got("pts_p", d, slot)
        rdma("pts_d", d, slot, slot, twin).start()

    loop(1, np_, pts_forward)
    loop(1, nz, lambda d: got("pts_z", d, ptsi.at[zfrom(d)]))
    got("pts_d", 0, ptsj.at[oc * np_ + p])
    loop(1, np_, lambda d: got("pts_d", d, ptsj.at[oc * np_ + plane_slot(d)]))

    for t in range(half):
        two = jnp.concatenate([ptsi[2 * t], ptsi[2 * t + 1]], 1)
        right[t] = exponent_right(two).astype(BF16)

    def kern_block(j):
        two = jnp.concatenate([ptsj[2 * j], ptsj[2 * j + 1]], 1)
        left = exponent_left(two).T.astype(BF16)
        row = pl.multiple_of(j * 2 * B, 2 * B)
        for t in range(half):
            kern[t, pl.ds(row, 2 * B), :] = jnp.exp2(mm(left, right[t])).astype(BF16)

    loop(0, np_, kern_block)

    both = jnp.concatenate([pts_ref[...], ptsj[oc * np_ + p]], 1)
    b1, b2, b3 = three_parts(both)
    none = jnp.zeros((64, 2 * B), F32)
    ones = rows_of((1.0, 1.0, 1.0), 2 * B)
    tail = none[:32]
    pside[0] = jnp.concatenate([none, b1, b1, b1, ones, tail], 0).astype(BF16)
    pside[1] = jnp.concatenate([none, b2, b2, none[:16], tail, none[:0]][:5], 0).astype(BF16)
    pside[2] = jnp.concatenate([none, b3, none[:24], tail], 0).astype(BF16)
    prior_s[...] = jnp.zeros_like(prior_s)

    def prior_chunk(i):
        def one_wait(dy):
            d = i * ny + dy
            got("prm_p", d, prm.at[plane_slot(d)])

        @pl.when(i == 0)
        def _():
            loop(1, ny, one_wait)

        @pl.when(i > 0)
        def _():
            loop(0, ny, one_wait)

        xx = lax.rem(x + nx - i, nx)
        part = prm[pl.ds(xx * ny, ny)].reshape(ny * half * FB, 128)
        turns = mm(part, pside[0]) + mm(part, pside[1]) + mm(part, pside[2])
        feats = cos_turns(turns)
        f1 = feats.astype(BF16)
        f2 = (feats - f1.astype(F32)).astype(BF16)
        flip = (((0,), (0,)), ((), ()))
        prior_s[...] += (mm(part, f1, flip) + mm(part, f2, flip))[:S]

    loop(0, nx, prior_chunk)

    outb[0, 0] = prior_s[:, B:]
    rdma("prior", 0, outb.at[0, 0], rcv.at[2, 0], twin).start()
    got("prior", 0, rcv.at[2, 0])
    scale = math.sqrt(2.0 / nfeat)
    prior = scale * (prior_s[:, :B] + rcv[2, 0])
    rhs = tgt_ref[...] - prior - 0.5 * noise_ref[...]
    rhs_s[0] = prior
    rhs_s[1] = rhs
    rdma("prior", 0, outb.at[0, 0], rcv.at[2, 0], twin).wait_send()

    def matvec(n, field, first, each, last):
        pn, dn, zn, on = "low%d_p" % n, "low%d_d" % n, "low%d_z" % n, "out%d" % n
        own = low.at[n, c * np_ + p]
        low[n, c * np_ + p] = field.astype(BF16)
        loop(1, np_, lambda d: rdma(pn, d, own, own, plane_dev(d)).start())
        rdma(dn, 0, own, own, twin).start()
        loop(1, nz, lambda d: rdma(zn, d, own, low_z.at[n, z], zdev(d, c)).start())
        low_z[n, z] = field.astype(BF16)
        first()

        def forward(d):
            slot = low.at[n, c * np_ + plane_slot(d)]
            got(pn, d, slot)
            rdma(dn, d, slot, slot, twin).start()

        loop(1, np_, forward)
        loop(1, nz, lambda d: got(zn, d, low_z.at[n, zfrom(d)]))
        got(dn, 0, low.at[n, oc * np_ + p])
        loop(1, np_, lambda d: got(dn, d, low.at[n, oc * np_ + plane_slot(d)]))

        fields = jnp.concatenate([low[n, j] for j in range(2 * np_)], 1)

        def tile(k):
            t = lax.rem(lax.div(z, 2) + half // 2 + k, half)
            out = mm(fields, kern[t])
            for s in range(2):
                zz = 2 * t + s
                piece = out[:, s * B:(s + 1) * B]
                outb[n, zz] = piece
                each(zz, piece)

                @pl.when(zz != z)
                def _():
                    d = lax.rem(zz + nz - z, nz)
                    rdma(on, d, outb.at[n, zz], rcv.at[n, z], (x, zz, y, c)).start()

        loop(0, half, tile)
        last()
        rcv[n, z] = outb[n, z]
        loop(1, nz, lambda d: got(on, d, rcv.at[n, zfrom(d)]))
        total = rcv[n, 0]
        for zz in range(1, nz):
            total = total + rcv[n, zz]
        return total

    def z_start(name, buf, value):
        zc = 2 * z + c
        buf[zc] = value
        rdma(name + "_z", 0, buf.at[zc], buf.at[zc], twin).start()

        def go(d):
            rdma(name + "_z", 2 * d, buf.at[zc], buf.at[zc], zdev(d, c)).start()
            rdma(name + "_z", 2 * d + 1, buf.at[zc], buf.at[zc], zdev(d, oc)).start()

        loop(1, nz, go)

    def z_end(name, buf):
        got(name + "_z", 0, buf.at[2 * z + oc])

        def come(d):
            got(name + "_z", 2 * d, buf.at[2 * zfrom(d) + c])
            got(name + "_z", 2 * d + 1, buf.at[2 * zfrom(d) + oc])

        loop(1, nz, come)
        total = buf[0]
        for k in range(1, 2 * nz):
            total = total + buf[k]
        return total

    def p_start(name, buf, value):
        buf[p] = value
        loop(1, np_, lambda d: rdma(name + "_p", d, buf.at[p], buf.at[p], plane_dev(d)).start())

    def p_end(name, buf):
        loop(1, np_, lambda d: got(name + "_p", d, buf.at[plane_slot(d)]))
        total = buf[0]
        for k in range(1, np_):
            total = total + buf[k]
        return total

    def spread(row):
        return jnp.broadcast_to(row, (128, 128)).T

    def lane_sums(arrays):
        return jnp.sum(jnp.concatenate(arrays, 0).T, 0, keepdims=True)

    def none_yet():
        pass

    acc[...] = jnp.zeros_like(acc)

    def each0(zz, piece):
        acc[0] += piece * low_z[0, zz].astype(F32)

    def last0():
        r = rhs_s[1]
        p_start("cur0", cur_p.at[0], lane_sums([acc[0], r * r]))

    k0 = matvec(0, rhs, none_yet, each0, last0)
    z_start("cur0", cur_z.at[0], p_end("cur0", cur_p.at[0]))
    rhs = rhs_s[1]
    q1 = k0 + JITTER * rhs
    rhs_s[2] = k0
    sums = spread(z_end("cur0", cur_z.at[0]))
    m0 = sums[S:]
    alpha = m0 / (sums[:S] + JITTER * m0)
    r1 = rhs - alpha * q1
    rhs_s[3] = r1
    rhs_s[4] = alpha
    rhs_s[5] = m0

    acc[...] = jnp.zeros_like(acc)

    def first1():
        r, k, new = rhs_s[1], rhs_s[2], rhs_s[3]
        sums = lane_sums([new * new, new * r, new * k, r * k])
        z_start("mom", mom_z, jnp.concatenate([sums[:, :128], sums[:, 128:]], 0))

    def each1(zz, piece):
        acc[0] += piece * low_z[1, zz].astype(F32)
        acc[1] += piece * low_z[0, zz].astype(F32)

    def last1():
        p_start("cur1", cur_p.at[1], lane_sums([acc[0], acc[1]]))
        p_start("mom", mom_p, z_end("mom", mom_z))
        z_start("cur1", cur_z.at[1], p_end("cur1", cur_p.at[1]))

    k1 = matvec(1, r1, first1, each1, last1)
    prior, r, k0, r1, alpha, m0 = (rhs_s[k] for k in range(6))
    mom = p_end("mom", mom_p)
    one, two = spread(mom[0:1]), spread(mom[1:2])
    n1, r1r, r1k, rk = one[:S], one[S:], two[:S], two[S:]
    beta = n1 / m0
    kd = k1 + beta * k0
    dire = r1 + beta * r
    dd = n1 + beta * (2.0 * r1r + beta * m0)
    part = spread(z_end("cur1", cur_z.at[1]))
    curve = part[:S] + beta * part[S:] + beta * (r1k + beta * rk) + JITTER * dd
    alpha2 = n1 / curve
    post_ref[...] = prior + alpha * k0 + alpha2 * kd
    res_ref[...] = r1 - alpha2 * (kd + JITTER * dire)

    def sent(name, k, src):
        rdma(name, k, src, src, twin).wait_send()

    @pl.when(mine)
    def _():
        loop(1, nz, lambda d: sent("prm_z", d, prm_ref))

    def plane_sent(d):
        sent("prm_p", d, prm.at[p])
        sent("pts_p", d, pts_ref)
        sent("pts_d", d, pts_ref)
        for n in range(2):
            sent("low%d_p" % n, d, low.at[n, p])
            sent("low%d_d" % n, d, low.at[n, p])
            sent("cur%d_p" % n, d, cur_p.at[n, p])
        sent("mom_p", d, mom_p.at[p])

    loop(1, np_, plane_sent)
    sent("pts_d", 0, pts_ref)
    for n in range(2):
        sent("low%d_d" % n, 0, low.at[n, p])
        sent("cur%d_z" % n, 0, cur_z.at[n, z])
    sent("mom_z", 0, mom_z.at[z])

    def z_sent(d):
        sent("pts_z", d, pts_ref)
        for n in range(2):
            sent("low%d_z" % n, d, low.at[n, p])
            sent("out%d" % n, d, outb.at[n, z])
            for s in range(2):
                sent("cur%d_z" % n, 2 * d + s, cur_z.at[n, z])
        for s in range(2):
            sent("mom_z", 2 * d + s, mom_z.at[z])

    loop(1, nz, z_sent)


def body(sizes, points, targets, noise, omega, phase, weights):
    nx, nz, ny = sizes
    np_, half = nx * ny, nz // 2

    def cut(a):
        return lax.reduce_precision(a, 8, 7)

    turn = 1.0 / (2.0 * math.pi)
    parts = [weights]
    for v in (omega.T * turn, phase[:, None] * turn):
        one = cut(v)
        two = cut(v - one)
        parts.append((one, two, cut(v - one - two)))
    flat = [parts[0], *parts[1], *parts[2], jnp.zeros((FB, 128 - S - 3 * D - 3), F32)]
    packed = jnp.concatenate(flat, 1).astype(BF16)

    vmem = pl.BlockSpec(memory_space=pltpu.VMEM)
    sems = sum(count for _, count in SLOTS(nz, np_))
    block = jax.ShapeDtypeStruct((S, B), F32)
    return pl.pallas_call(
        functools.partial(kernel, sizes),
        out_shape=(block, block),
        in_specs=[vmem] * 4,
        out_specs=(vmem, vmem),
        scratch_shapes=[
            pltpu.VMEM((np_, half, FB, 128), BF16),
            pltpu.VMEM((2 * np_, D, B), F32),
            pltpu.VMEM((nz, D, B), F32),
            pltpu.VMEM((3, 128, 2 * B), BF16),
            pltpu.VMEM((S, 2 * B), F32),
            pltpu.VMEM((2, S, B), F32),
            pltpu.VMEM((6, S, B), F32),
            pltpu.VMEM((2, 2 * np_, S, B), BF16),
            pltpu.VMEM((2, nz, S, B), BF16),
            pltpu.VMEM((half, 64, 2 * B), BF16),
            pltpu.VMEM((half, 2 * np_ * B, 2 * B), BF16),
            pltpu.VMEM((2, nz, S, B), F32),
            pltpu.VMEM((3, nz, S, B), F32),
            pltpu.VMEM((2 * nz, 2, 128), F32),
            pltpu.VMEM((np_, 2, 128), F32),
            pltpu.VMEM((2, 2 * nz, 1, 128), F32),
            pltpu.VMEM((2, np_, 1, 128), F32),
            pltpu.SemaphoreType.DMA((sems,)),
            pltpu.SemaphoreType.DMA((sems,)),
        ],
        compiler_params=pltpu.CompilerParams(
            collective_id=0, has_side_effects=True, vmem_limit_bytes=40 * 1024 * 1024),
    )(points, targets[None, :], noise, packed)


def build(mesh, sizes):
    finer = Mesh(mesh.devices.reshape(*sizes, mesh.shape["cols"]), AXES)
    in_specs = (
        P(None, COLS_ROWS),
        P(COLS_ROWS),
        P(None, COLS_ROWS),
        P(None, ROWS),
        P(ROWS),
        P(ROWS, None),
    )
    out_specs = (P(None, COLS_ROWS), P(None, COLS_ROWS))
    return jax.shard_map(
        functools.partial(body, sizes), mesh=finer, in_specs=in_specs, out_specs=out_specs,
        check_vma=False)


def solution(mesh):
    return build(mesh, (4, 8, 4))
```

```python
import functools
import math

import jax
import jax.numpy as jnp
from jax import lax
from jax.experimental import pallas as pl
from jax.experimental.pallas import tpu as pltpu
from jax.sharding import Mesh
from jax.sharding import PartitionSpec as P

AXES = ("px", "pz", "py", "cols")
ROWS = ("px", "pz", "py")
COLS_ROWS = ("cols", "px", "pz", "py")
MESH = pl.DeviceIdType.MESH
F32, BF16 = jnp.float32, jnp.bfloat16

D = 8
S = 64
B = 128
FB = 16
JITTER = 0.25
KERN_EARLY = 10
SPREAD = math.sqrt(4.0 * math.log2(math.e))
SINE = [(-1) ** k * (2.0 * math.pi) ** (2 * k + 1) / math.factorial(2 * k + 1) for k in range(6)]


def SENDS():
    table = ["prm_z", "prm0", "prm1", "pts_z", "pts_p", "pts_d", "pts_o", "prior", "mom_z", "mom_p"]
    for n in "01":
        table += ["low%s_p" % n, "low%s_d" % n, "low%s_z" % n, "out%s" % n, "cur%s_z" % n, "cur%s_p" % n]
    return table


def RECVS(nx):
    several = {"prm_z": 4}
    for name in ("prm0", "prm1", "low0_p", "low0_d", "low1_p", "low1_d"):
        several[name] = nx
    return [(name, several.get(name, 1)) for name in SENDS()]


def three_parts(a):
    one = a.astype(BF16).astype(F32)
    rest = a - one
    two = rest.astype(BF16).astype(F32)
    three = (rest - two).astype(BF16).astype(F32)
    return one, two, three


def rows_of(pieces, width):
    row = lax.broadcasted_iota(jnp.int32, (8, width), 0)
    out = jnp.zeros((8, width), F32)
    for k, piece in enumerate(pieces):
        out = jnp.where(row == k, piece, out)
    return out


def exponent_left(points):
    scaled = points * SPREAD
    a1, a2, a3 = three_parts(scaled)
    n1, n2, n3 = three_parts(-0.5 * jnp.sum(scaled * scaled, 0, keepdims=True))
    width = points.shape[1]
    norms = rows_of((n1, n2, n3, 1.0, 1.0, 1.0), width)
    return jnp.concatenate([a1, a1, a2, a2, a1, a3, norms, jnp.zeros((8, width), F32)], 0)


def exponent_right(points):
    scaled = points * SPREAD
    b1, b2, b3 = three_parts(scaled)
    n1, n2, n3 = three_parts(-0.5 * jnp.sum(scaled * scaled, 0, keepdims=True))
    width = points.shape[1]
    norms = rows_of((1.0, 1.0, 1.0, n1, n2, n3), width)
    return jnp.concatenate([b1, b2, b1, b2, b3, b1, norms, jnp.zeros((8, width), F32)], 0)


def cos_turns(t):
    r = t - jnp.floor(t + 0.5)
    v = 0.25 - jnp.abs(r)
    w = v * v
    acc = jnp.full_like(w, SINE[-1])
    for c in SINE[-2::-1]:
        acc = acc * w + c
    return acc * v


def mm(a, b, dims=(((1,), (0,)), ((), ()))):
    return lax.dot_general(a, b, dims, preferred_element_type=F32)


def kernel(
    sizes,
    pts_hbm, tgt_hbm, noise_hbm, omega_hbm, phase_hbm, weights_hbm,
    post_ref, res_ref,
    pts, tgt, noise, omega, phase, weights,
    prm_own, bundle, ptw, ptsj, ptsi, pside, prior_s, halves, acc, rhs_s, low, low_z, right, kern, outb, rcv,
    mom_z, mom_p, cur_z, cur_p, send, recv, local,
):
    nx, nz, ny = sizes
    np_, half = nx * ny, nz // 2
    nfeat = nx * nz * ny * FB
    x, z, y, c = (lax.axis_index(a) for a in AXES)
    xs = [x] + [lax.rem(x + d, nx) for d in range(1, nx)]
    ys = [y] + [lax.rem(y + d, ny) for d in range(1, ny)]
    zs = [z] + [lax.rem(z + d, nz) for d in range(1, nz)]
    p = x * ny + y
    oc = 1 - c
    twin = (x, z, y, oc)

    arrivals = []
    for k, (src, dst) in enumerate((
        (weights_hbm, weights), (omega_hbm, omega), (phase_hbm, phase), (pts_hbm, pts),
        (tgt_hbm, tgt), (noise_hbm, noise),
    )):
        copy = pltpu.make_async_copy(src, dst, local.at[k])
        copy.start()
        arrivals.append(copy)

    at = {}
    top = 0
    for name, count in RECVS(nx):
        at[name] = top
        top += count
    order = {name: k for k, name in enumerate(SENDS())}

    def rdma(name, k, src, dst, dev):
        return pltpu.make_async_remote_copy(
            src_ref=src, dst_ref=dst, send_sem=send.at[order[name]], recv_sem=recv.at[at[name] + k],
            device_id=dev, device_id_type=MESH)

    pending = []

    def put(name, k, src, dst, dev):
        rdma(name, k, src, dst, dev).start()

    def sent(name, whole):
        pending.append((name, whole))

    def flush():
        for name, whole in pending:
            rdma(name, 0, whole, whole, twin).wait_send()
        pending.clear()

    def got(name, k, dst):
        rdma(name, k, dst, dst, twin).wait_recv()

    def hops(d, n):
        return min(d, n - d)

    def dxy(d):
        return d // ny, d % ny

    near_p = sorted(range(1, np_), key=lambda d: hops(d // ny, nx) + hops(d % ny, ny))
    far_p = near_p[::-1]
    near_z = sorted(range(1, nz), key=lambda d: hops(d, nz))
    far_z = near_z[::-1]

    def plane_dev(d):
        dx, dy = dxy(d)
        return (xs[dx], z, ys[dy], c)

    def plane_slot(d):
        dx, dy = dxy(d)
        return xs[(nx - dx) % nx] * ny + ys[(ny - dy) % ny]

    def zdev(d, core):
        return (x, zs[d], y, core)

    def zfrom(d):
        return zs[(nz - d) % nz]

    with jax.named_scope("a_barrier"):
        bar = pltpu.get_barrier_semaphore()

        def greet(dev):
            pl.semaphore_signal(bar, inc=1, device_id=dev, device_id_type=MESH)

        for d in far_p:
            greet(plane_dev(d))
        for d in far_z:
            greet(zdev(d, c))
            greet(zdev(d, oc))
        greet(twin)

        turn = 1.0 / (2.0 * math.pi)
        for copy in arrivals[:4]:
            copy.wait()
        lane = lax.broadcasted_iota(jnp.int32, (FB, 128), 1)
        row = lax.broadcasted_iota(jnp.int32, (FB, 128), 0)
        angles = jnp.concatenate([omega[...], phase[...], jnp.zeros((FB - D - 1, FB), F32)], 0) * turn
        packed = jnp.zeros((FB, 128), F32)
        flip = (((0,), (0,)), ((), ()))
        for k, piece in enumerate(three_parts(angles)):
            spot = jnp.where(row < D, S + k * D + row, S + 3 * D + k)
            pick = jnp.where((lane == spot) & (row <= D), 1.0, 0.0)
            packed = packed + mm(piece.astype(BF16), pick.astype(BF16), flip)
        w1 = weights[...].astype(BF16)
        w2 = (weights[...] - w1.astype(F32)).astype(BF16)
        wide = lax.broadcasted_iota(jnp.int32, (S, 128), 1)
        deep = lax.broadcasted_iota(jnp.int32, (S, 128), 0)
        once = jnp.where(wide == deep, 1.0, 0.0).astype(BF16)
        twice = jnp.where((wide == deep) | (wide == deep + S), 1.0, 0.0).astype(BF16)
        prm_own[0] = (packed + mm(w1, once)).astype(BF16)
        prm_own[1] = mm(w2, twice).astype(BF16)
        pl.semaphore_wait(bar, 1 + 2 * (nz - 1) + np_ - 1)

    mine = lax.rem(z, 2) == c
    zslot = lax.div(z, 2)

    with jax.named_scope("b_prm_z"):
        par = lax.rem(z + c, 2)
        turnout = {1: 0, 7: 1, 3: 2, 5: 3, 2: 1, 6: 2, 4: 3}
        places = [par, 2 + 5 * par, 6 - 3 * par, 4 + par]

        @pl.when(mine)
        def _():
            for d in far_z:
                put("prm_z", turnout[d], prm_own, halves.at[d], zdev(d, c))
            halves[0] = prm_own[...]

        put("pts_o", 0, pts, ptw, twin)
        sent("pts_o", pts)
        for d in far_p:
            put("pts_p", 0, pts, ptsj.at[c * np_ + p], plane_dev(d))
        for d in far_z:
            put("pts_z", 0, pts, ptsi.at[z], zdev(d, c))
        sent("pts_p", ptsj.at[pl.ds(0, np_ - 1)])
        sent("pts_z", ptsi.at[pl.ds(0, nz - 1)])
        ptsj[c * np_ + p] = pts[...]
        ptsi[z] = pts[...]

        left_lanes = lax.broadcasted_iota(jnp.int32, (FB, 128), 1) < S
        for stage in range(2):
            if stage == 0:
                @pl.when(jnp.logical_not(mine))
                def _():
                    got("prm_z", 0, halves.at[1])
            else:
                got("prm_z", 2, halves.at[places[2]])
            got("prm_z", 2 * stage + 1, halves.at[places[2 * stage + 1]])
            one, two = halves[places[2 * stage]], halves[places[2 * stage + 1]]
            bundle[stage, p, 0] = one[0]
            bundle[stage, p, 1] = two[0]
            bundle[stage, p, 2] = jnp.where(left_lanes, one[1].astype(F32), two[1].astype(F32)).astype(BF16)
            name = "prm%d" % stage
            for d in far_p:
                put(name, d // ny, bundle.at[stage, p], bundle.at[stage, p], plane_dev(d))
            sent(name, bundle.at[stage, pl.ds(0, np_ - 1)])

    with jax.named_scope("c_points"):
        got("pts_o", 0, ptw)
        got("pts_p", 0, ptsj.at[pl.ds(0, np_ - 1)])
        here = ptsj.at[pl.ds(c * np_, np_)]
        put("pts_d", 0, here, here, twin)
        sent("pts_d", here)
        got("pts_z", 0, ptsi.at[pl.ds(0, nz - 1)])
        both = jnp.concatenate([pts[...], ptw[...]], 1)
        b1, b2, b3 = three_parts(both)
        none = jnp.zeros((S, 2 * B), F32)
        ones = rows_of((1.0, 1.0, 1.0), 2 * B)
        pside[0] = jnp.concatenate([none, b1, b1, b1, ones, none[:32]], 0).astype(BF16)
        pside[1] = jnp.concatenate([none, b2, b2, none[:48]], 0).astype(BF16)
        pside[2] = jnp.concatenate([none, b3, none[:56]], 0).astype(BF16)
        prior_s[...] = jnp.zeros_like(prior_s)
        for t in range(half):
            two = jnp.concatenate([ptsi[2 * t], ptsi[2 * t + 1]], 1)
            right[t] = exponent_right(two).astype(BF16)
        got("pts_d", 0, ptsj.at[pl.ds(oc * np_, np_)])

    def kern_block(j, carry):
        two = jnp.concatenate([ptsj[2 * j], ptsj[2 * j + 1]], 1)
        left = exponent_left(two).T.astype(BF16)
        row = pl.multiple_of(j * 2 * B, 2 * B)
        for t in range(half):
            kern[t, pl.ds(row, 2 * B), :] = jnp.exp2(mm(left, right[t])).astype(BF16)
        return carry

    early = (np_ * KERN_EARLY) // 16
    with jax.named_scope("d_kern"):
        lax.fori_loop(0, early, kern_block, 0)

    with jax.named_scope("e_prior"):
        for dx in sorted(range(nx), key=lambda d: hops(d, nx)):
            base = xs[(nx - dx) % nx] * ny
            for stage in range(2):
                group = bundle.at[stage, pl.ds(0, ny - 1)] if dx == 0 else bundle.at[stage, pl.ds(base, ny)]
                got("prm%d" % stage, dx, group)
                part = jnp.concatenate([bundle[stage, base + q, k] for k in range(2) for q in range(ny)], 0)
                rest = jnp.concatenate([bundle[stage, base + q, 2] for q in range(ny)], 0)
                cut = ny * FB
                turns = mm(part, pside[0]) + mm(part, pside[1]) + mm(part, pside[2])
                feats = cos_turns(turns)
                f1 = feats.astype(BF16)
                f2 = (feats - f1.astype(F32)).astype(BF16)
                total = (mm(part, f1, flip) + mm(part, f2, flip))[:S]
                prior_s[...] += total + mm(rest, f1[:cut], flip)[:S] + mm(rest, f1[cut:], flip)[S:]

    with jax.named_scope("f_swap"):
        rcv[2, 1] = prior_s[:, B:]
        put("prior", 0, rcv.at[2, 1], rcv.at[2, 0], twin)
        sent("prior", rcv.at[2, 1])
        for copy in arrivals[4:]:
            copy.wait()
        got("prior", 0, rcv.at[2, 0])
        scale = math.sqrt(2.0 / nfeat)
        prior = scale * (prior_s[:, :B] + rcv[2, 0])
        rhs = tgt[...] - prior - 0.5 * noise[...]
        rhs_s[0] = prior
        rhs_s[1] = rhs
        low[0, c * np_ + p] = rhs.astype(BF16)
        low_z[0, z] = rhs.astype(BF16)

    def matvec(n, first, each, last):
        pn, dn, zn, on = "low%d_p" % n, "low%d_d" % n, "low%d_z" % n, "out%d" % n
        own = low.at[n, c * np_ + p]
        with jax.named_scope("g%d_send" % n):
            for d in far_p:
                put(pn, d // ny, own, own, plane_dev(d))
            for d in far_z:
                put(zn, 0, own, low_z.at[n, z], zdev(d, c))
            sent(pn, low.at[n, pl.ds(0, np_ - 1)])
            sent(zn, low_z.at[n, pl.ds(0, nz - 1)])
            sent(dn, low.at[n, pl.ds(0, np_)])
        with jax.named_scope("h%d_first" % n):
            first()

        def group_of(core, dx):
            return low.at[n, pl.ds(core * np_ + xs[(nx - dx) % nx] * ny, ny)]

        def own_group(dx):
            group = group_of(c, dx)
            got(pn, dx, low.at[n, pl.ds(0, ny - 1)] if dx == 0 else group)
            put(dn, dx, group, group, twin)

        def twin_group(dx):
            got(dn, dx, group_of(oc, dx))

        def times(core, dx, t):
            base = core * np_ + xs[(nx - dx) % nx] * ny
            fields = jnp.concatenate([low[n, base + q] for q in range(ny)], 1)
            row = pl.multiple_of(base * B, B * ny)
            return mm(fields, kern[t, pl.ds(row, B * ny), :])

        def add_tiles(groups, fresh):
            def tile(t, carry):
                out = times(*groups[0], t)
                for group in groups[1:]:
                    out = out + times(*group, t)
                for s in range(2):
                    piece = out[:, s * B:(s + 1) * B]
                    zz = 2 * t + s
                    outb[n, zz] = piece if fresh else outb[n, zz] + piece
                return carry

            lax.fori_loop(0, half, tile, 0)

        spans = sorted(range(nx), key=lambda d: hops(d, nx))
        with jax.named_scope("i%d_gather" % n):
            own_group(spans[0])
            own_group(spans[1])
            add_tiles([(c, spans[0]), (c, spans[1])], True)
            own_group(spans[2])
            got(zn, 0, low_z.at[n, pl.ds(0, nz - 1)])
            twin_group(spans[0])
            twin_group(spans[1])
            add_tiles([(oc, spans[0]), (oc, spans[1])], False)
            own_group(spans[3])
            twin_group(spans[2])
            add_tiles([(c, spans[2]), (c, spans[3]), (oc, spans[2])], False)
            twin_group(spans[3])
            flush()

        with jax.named_scope("j%d_tiles" % n):
            for k in range(half):
                t = lax.rem(zslot + half // 2 + k, half)
                out = times(oc, spans[3], t)
                for s in range(2):
                    zz = 2 * t + s
                    piece = outb[n, zz] + out[:, s * B:(s + 1) * B]
                    outb[n, zz] = piece
                    each(zz, piece)
                if k == half - half // 2 or half == 1:
                    targets = [z + 1 - 2 * lax.rem(z, 2)]
                else:
                    targets = [2 * t, 2 * t + 1]
                for zz in targets:
                    put(on, 0, outb.at[n, zz], rcv.at[n, z], (x, zz, y, c))
            sent(on, outb.at[n, pl.ds(0, nz - 1)])
        with jax.named_scope("k%d_last" % n):
            last()
        with jax.named_scope("l%d_reduce" % n):
            total = outb[n, z]
            got(on, 0, rcv.at[n, pl.ds(0, nz - 1)])
            for d in near_z:
                total = total + rcv[n, zfrom(d)]
        return total

    def z_start(name, buf, value):
        zc = 2 * z + c
        buf[zc] = value
        for d in far_z:
            put(name + "_z", 0, buf.at[zc], buf.at[zc], zdev(d, c))
            put(name + "_z", 0, buf.at[zc], buf.at[zc], zdev(d, oc))
        put(name + "_z", 0, buf.at[zc], buf.at[zc], twin)
        sent(name + "_z", buf.at[pl.ds(0, 2 * nz - 1)])

    def z_end(name, buf):
        got(name + "_z", 0, buf.at[pl.ds(0, 2 * nz - 1)])
        return sum_all(buf, 2 * nz)

    def p_start(name, buf, value):
        buf[p] = value
        for d in far_p:
            put(name + "_p", 0, buf.at[p], buf.at[p], plane_dev(d))
        sent(name + "_p", buf.at[pl.ds(0, np_ - 1)])

    def p_end(name, buf):
        got(name + "_p", 0, buf.at[pl.ds(0, np_ - 1)])
        return sum_all(buf, np_)

    def sum_all(buf, count):
        parts = [buf[k] for k in range(count)]
        while len(parts) > 1:
            parts = [a + b for a, b in zip(parts[::2], parts[1::2])]
        return parts[0]

    def spread(row):
        return jnp.broadcast_to(row, (128, 128)).T

    def lane_sums(arrays):
        return jnp.sum(jnp.concatenate(arrays, 0).T, 0, keepdims=True)

    acc[...] = jnp.zeros_like(acc)

    def first0():
        lax.fori_loop(early, np_, kern_block, 0)

    def each0(zz, piece):
        acc[0] += piece * low_z[0, zz].astype(F32)

    def last0():
        r = rhs_s[1]
        p_start("cur0", cur_p.at[0], lane_sums([acc[0], r * r]))
        z_start("cur0", cur_z.at[0], p_end("cur0", cur_p.at[0]))

    k0 = matvec(0, first0, each0, last0)
    with jax.named_scope("m_alpha"):
        rhs = rhs_s[1]
        q1 = k0 + JITTER * rhs
        rhs_s[2] = k0
        acc[...] = jnp.zeros_like(acc)
        sums = spread(z_end("cur0", cur_z.at[0]))
        m0 = sums[S:]
        alpha = m0 / (sums[:S] + JITTER * m0)
        r1 = rhs - alpha * q1
        low[1, c * np_ + p] = r1.astype(BF16)
        low_z[1, z] = r1.astype(BF16)
        rhs_s[3] = r1
        rhs_s[4] = alpha
        rhs_s[5] = m0

    def first1():
        r, k, new = rhs_s[1], rhs_s[2], rhs_s[3]
        sums = lane_sums([new * new, new * r, new * k, r * k])
        z_start("mom", mom_z, jnp.concatenate([sums[:, :128], sums[:, 128:]], 0))

    def each1(zz, piece):
        acc[0] += piece * low_z[1, zz].astype(F32)
        acc[1] += piece * low_z[0, zz].astype(F32)

    def last1():
        p_start("cur1", cur_p.at[1], lane_sums([acc[0], acc[1]]))
        p_start("mom", mom_p, z_end("mom", mom_z))
        z_start("cur1", cur_z.at[1], p_end("cur1", cur_p.at[1]))

    k1 = matvec(1, first1, each1, last1)
    with jax.named_scope("n_finish"):
        prior, r, k0, r1, alpha, m0 = (rhs_s[k] for k in range(6))
        mom = p_end("mom", mom_p)
        one, two = spread(mom[0:1]), spread(mom[1:2])
        n1, r1r, r1k, rk = one[:S], one[S:], two[:S], two[S:]
        beta = n1 / m0
        kd = k1 + beta * k0
        dire = r1 + beta * r
        dd = n1 + beta * (2.0 * r1r + beta * m0)
        known = beta * (r1k + beta * rk) + JITTER * dd
        part = spread(z_end("cur1", cur_z.at[1]))
        alpha2 = n1 / (part[:S] + beta * part[S:] + known)
        post_ref[...] = prior + alpha * k0 + alpha2 * kd
        res_ref[...] = r1 - alpha2 * (kd + JITTER * dire)

        flush()

        @pl.when(mine)
        def _():
            whole = halves.at[pl.ds(0, nz - 1)]
            rdma("prm_z", 0, whole, whole, twin).wait_send()


def body(sizes, points, targets, noise, omega, phase, weights):
    nx, nz, ny = sizes
    np_, half = nx * ny, nz // 2
    vmem = pl.BlockSpec(memory_space=pltpu.VMEM)
    hbm = pl.BlockSpec(memory_space=pltpu.HBM)
    block = pltpu.VMEM((S, B), F32)
    return pl.pallas_call(
        functools.partial(kernel, sizes),
        out_shape=(block, block),
        in_specs=[hbm] * 6,
        out_specs=(vmem, vmem),
        scratch_shapes=[
            pltpu.VMEM((D, B), F32),
            pltpu.VMEM((1, B), F32),
            pltpu.VMEM((S, B), F32),
            pltpu.VMEM((D, FB), F32),
            pltpu.VMEM((1, FB), F32),
            pltpu.VMEM((FB, S), F32),
            pltpu.VMEM((2, FB, 128), BF16),
            pltpu.VMEM((2, np_, 3, FB, 128), BF16),
            pltpu.VMEM((D, B), F32),
            pltpu.VMEM((2 * np_, D, B), F32),
            pltpu.VMEM((nz, D, B), F32),
            pltpu.VMEM((3, 128, 2 * B), BF16),
            pltpu.VMEM((S, 2 * B), F32),
            pltpu.VMEM((nz, 2, FB, 128), BF16),
            pltpu.VMEM((2, S, B), F32),
            pltpu.VMEM((6, S, B), F32),
            pltpu.VMEM((2, 2 * np_, S, B), BF16),
            pltpu.VMEM((2, nz, S, B), BF16),
            pltpu.VMEM((half, 64, 2 * B), BF16),
            pltpu.VMEM((half, 2 * np_ * B, 2 * B), BF16),
            pltpu.VMEM((2, nz, S, B), F32),
            pltpu.VMEM((3, nz, S, B), F32),
            pltpu.VMEM((2 * nz, 2, 128), F32),
            pltpu.VMEM((np_, 2, 128), F32),
            pltpu.VMEM((2, 2 * nz, 1, 128), F32),
            pltpu.VMEM((2, np_, 1, 128), F32),
            pltpu.SemaphoreType.DMA((len(SENDS()),)),
            pltpu.SemaphoreType.DMA((sum(count for _, count in RECVS(nx)),)),
            pltpu.SemaphoreType.DMA((6,)),
        ],
        compiler_params=pltpu.CompilerParams(
            collective_id=0, has_side_effects=True, vmem_limit_bytes=62000000),
    )(points, targets[None, :], noise, omega, phase[None, :], weights)


def build(mesh, sizes):
    finer = Mesh(mesh.devices.reshape(*sizes, mesh.shape["cols"]), AXES)
    in_specs = (
        P(None, COLS_ROWS),
        P(COLS_ROWS),
        P(None, COLS_ROWS),
        P(None, ROWS),
        P(ROWS),
        P(ROWS, None),
    )
    out_specs = (P(None, COLS_ROWS), P(None, COLS_ROWS))
    return jax.shard_map(
        functools.partial(body, sizes), mesh=finer, in_specs=in_specs, out_specs=out_specs,
        check_vma=False)


def solution(mesh):
    return build(mesh, (4, 8, 4))
```

```python
import functools
import math

import jax
import jax.numpy as jnp
from jax import lax
from jax.experimental import pallas as pl
from jax.experimental.pallas import tpu as pltpu
from jax.sharding import Mesh
from jax.sharding import PartitionSpec as P

AXES = ("px", "pz", "py", "cols")
ROWS = ("px", "pz", "py")
COLS_ROWS = ("cols", "px", "pz", "py")
MESH = pl.DeviceIdType.MESH
F32, BF16 = jnp.float32, jnp.bfloat16

D = 8
S = 64
B = 128
FB = 16
JITTER = 0.25
KERN_EARLY = 7
SPREAD = math.sqrt(4.0 * math.log2(math.e))
SINE = [(-1) ** k * (2.0 * math.pi) ** (2 * k + 1) / math.factorial(2 * k + 1) for k in range(6)]


def SENDS():
    table = ["prm_z", "prm0", "prm1", "pts_z", "pts_p", "pts_d", "pts_o", "prior", "mom_z", "mom_p"]
    for n in "01":
        table += ["low%s_p" % n, "low%s_d" % n, "low%s_z" % n, "out%s" % n, "cur%s_z" % n, "cur%s_p" % n]
    return table


def RECVS(nx):
    several = {"prm_z": 4}
    for name in ("prm0", "prm1", "low0_p", "low0_d", "low1_p", "low1_d"):
        several[name] = nx
    return [(name, several.get(name, 1)) for name in SENDS()]


def three_parts(a):
    one = a.astype(BF16).astype(F32)
    rest = a - one
    two = rest.astype(BF16).astype(F32)
    three = (rest - two).astype(BF16).astype(F32)
    return one, two, three


def rows_of(pieces, width):
    row = lax.broadcasted_iota(jnp.int32, (8, width), 0)
    out = jnp.zeros((8, width), F32)
    for k, piece in enumerate(pieces):
        out = jnp.where(row == k, piece, out)
    return out


def exponent_left(points):
    scaled = points * SPREAD
    a1, a2, a3 = three_parts(scaled)
    n1, n2, n3 = three_parts(-0.5 * jnp.sum(scaled * scaled, 0, keepdims=True))
    width = points.shape[1]
    norms = rows_of((n1, n2, n3, 1.0, 1.0, 1.0), width)
    return jnp.concatenate([a1, a1, a2, a2, a1, a3, norms, jnp.zeros((8, width), F32)], 0)


def exponent_right(points):
    scaled = points * SPREAD
    b1, b2, b3 = three_parts(scaled)
    n1, n2, n3 = three_parts(-0.5 * jnp.sum(scaled * scaled, 0, keepdims=True))
    width = points.shape[1]
    norms = rows_of((1.0, 1.0, 1.0, n1, n2, n3), width)
    return jnp.concatenate([b1, b2, b1, b2, b3, b1, norms, jnp.zeros((8, width), F32)], 0)


def cos_turns(t):
    r = t - jnp.floor(t + 0.5)
    v = 0.25 - jnp.abs(r)
    w = v * v
    acc = jnp.full_like(w, SINE[-1])
    for c in SINE[-2::-1]:
        acc = acc * w + c
    return acc * v


def mm(a, b, dims=(((1,), (0,)), ((), ()))):
    return lax.dot_general(a, b, dims, preferred_element_type=F32)


def kernel(
    sizes,
    pts_hbm, tgt_hbm, noise_hbm, omega_hbm, phase_hbm, weights_hbm,
    out_ref,
    pts, tgt, noise, omega, phase, weights,
    prm_own, bundle, ptw, ptsj, ptsi, pside, prior_s, halves, rhs_s, low, low_z, right, kern, outb, rcv,
    mom_z, mom_p, cur_z, cur_p, send, recv, local,
):
    nx, nz, ny = sizes
    np_, half = nx * ny, nz // 2
    nfeat = nx * nz * ny * FB
    x, z, y, c = (lax.axis_index(a) for a in AXES)
    xs = [x] + [lax.rem(x + d, nx) for d in range(1, nx)]
    ys = [y] + [lax.rem(y + d, ny) for d in range(1, ny)]
    zs = [z] + [lax.rem(z + d, nz) for d in range(1, nz)]
    p = x * ny + y
    oc = 1 - c
    twin = (x, z, y, oc)

    arrivals = []
    for k, (src, dst) in enumerate((
        (weights_hbm, weights), (omega_hbm, omega), (phase_hbm, phase), (pts_hbm, pts),
        (tgt_hbm, tgt), (noise_hbm, noise),
    )):
        copy = pltpu.make_async_copy(src, dst, local.at[k])
        copy.start()
        arrivals.append(copy)

    at = {}
    top = 0
    for name, count in RECVS(nx):
        at[name] = top
        top += count
    order = {name: k for k, name in enumerate(SENDS())}

    def rdma(name, k, src, dst, dev):
        return pltpu.make_async_remote_copy(
            src_ref=src, dst_ref=dst, send_sem=send.at[order[name]], recv_sem=recv.at[at[name] + k],
            device_id=dev, device_id_type=MESH)

    pending = []

    def put(name, k, src, dst, dev):
        rdma(name, k, src, dst, dev).start()

    def sent(name, whole):
        pending.append((name, whole))

    def flush():
        for name, whole in pending:
            rdma(name, 0, whole, whole, twin).wait_send()
        pending.clear()

    def got(name, k, dst):
        rdma(name, k, dst, dst, twin).wait_recv()

    def hops(d, n):
        return min(d, n - d)

    def dxy(d):
        return d // ny, d % ny

    near_p = sorted(range(1, np_), key=lambda d: hops(d // ny, nx) + hops(d % ny, ny))
    far_p = near_p[::-1]
    near_z = sorted(range(1, nz), key=lambda d: hops(d, nz))
    far_z = near_z[::-1]

    def plane_dev(d):
        dx, dy = dxy(d)
        return (xs[dx], z, ys[dy], c)

    def plane_slot(d):
        dx, dy = dxy(d)
        return xs[(nx - dx) % nx] * ny + ys[(ny - dy) % ny]

    def zdev(d, core):
        return (x, zs[d], y, core)

    def zfrom(d):
        return zs[(nz - d) % nz]

    with jax.named_scope("a_barrier"):
        bar = pltpu.get_barrier_semaphore()

        def greet(dev):
            pl.semaphore_signal(bar, inc=1, device_id=dev, device_id_type=MESH)

        for d in far_p:
            greet(plane_dev(d))
        for d in far_z:
            greet(zdev(d, c))
            greet(zdev(d, oc))
        greet(twin)

        turn = 1.0 / (2.0 * math.pi)
        for copy in arrivals[:4]:
            copy.wait()
        lane = lax.broadcasted_iota(jnp.int32, (FB, 128), 1)
        row = lax.broadcasted_iota(jnp.int32, (FB, 128), 0)
        angles = jnp.concatenate([omega[...], phase[...], jnp.zeros((FB - D - 1, FB), F32)], 0) * turn
        packed = jnp.zeros((FB, 128), F32)
        flip = (((0,), (0,)), ((), ()))
        for k, piece in enumerate(three_parts(angles)):
            spot = jnp.where(row < D, S + k * D + row, S + 3 * D + k)
            pick = jnp.where((lane == spot) & (row <= D), 1.0, 0.0)
            packed = packed + mm(piece.astype(BF16), pick.astype(BF16), flip)
        w1 = weights[...].astype(BF16)
        w2 = (weights[...] - w1.astype(F32)).astype(BF16)
        wide = lax.broadcasted_iota(jnp.int32, (S, 128), 1)
        deep = lax.broadcasted_iota(jnp.int32, (S, 128), 0)
        once = jnp.where(wide == deep, 1.0, 0.0).astype(BF16)
        twice = jnp.where((wide == deep) | (wide == deep + S), 1.0, 0.0).astype(BF16)
        prm_own[0] = (packed + mm(w1, once)).astype(BF16)
        prm_own[1] = mm(w2, twice).astype(BF16)
        pl.semaphore_wait(bar, 1 + 2 * (nz - 1) + np_ - 1)

    mine = lax.rem(z, 2) == c
    zslot = lax.div(z, 2)

    with jax.named_scope("b_prm_z"):
        par = lax.rem(z + c, 2)
        turnout = {1: 0, 7: 1, 3: 2, 5: 3, 2: 1, 6: 2, 4: 3}
        places = [par, 2 + 5 * par, 6 - 3 * par, 4 + par]

        @pl.when(mine)
        def _():
            for d in far_z:
                put("prm_z", turnout[d], prm_own, halves.at[d], zdev(d, c))
            halves[0] = prm_own[...]

        put("pts_o", 0, pts, ptw, twin)
        sent("pts_o", pts)
        for d in far_p:
            put("pts_p", 0, pts, ptsj.at[c * np_ + p], plane_dev(d))
        for d in far_z:
            put("pts_z", 0, pts, ptsi.at[z], zdev(d, c))
        sent("pts_p", ptsj.at[pl.ds(0, np_ - 1)])
        sent("pts_z", ptsi.at[pl.ds(0, nz - 1)])
        ptsj[c * np_ + p] = pts[...]
        ptsi[z] = pts[...]

        left_lanes = lax.broadcasted_iota(jnp.int32, (FB, 128), 1) < S
        for stage in range(2):
            if stage == 0:
                @pl.when(jnp.logical_not(mine))
                def _():
                    got("prm_z", 0, halves.at[1])
            else:
                got("prm_z", 2, halves.at[places[2]])
            got("prm_z", 2 * stage + 1, halves.at[places[2 * stage + 1]])
            one, two = halves[places[2 * stage]], halves[places[2 * stage + 1]]
            bundle[stage, p, 0] = one[0]
            bundle[stage, p, 1] = two[0]
            bundle[stage, p, 2] = jnp.where(left_lanes, one[1].astype(F32), two[1].astype(F32)).astype(BF16)
            name = "prm%d" % stage
            for d in far_p:
                put(name, d // ny, bundle.at[stage, p], bundle.at[stage, p], plane_dev(d))
            sent(name, bundle.at[stage, pl.ds(0, np_ - 1)])

    with jax.named_scope("c_points"):
        got("pts_o", 0, ptw)
        got("pts_p", 0, ptsj.at[pl.ds(0, np_ - 1)])
        here = ptsj.at[pl.ds(c * np_, np_)]
        put("pts_d", 0, here, here, twin)
        sent("pts_d", here)
        got("pts_z", 0, ptsi.at[pl.ds(0, nz - 1)])
        both = jnp.concatenate([pts[...], ptw[...]], 1)
        b1, b2, b3 = three_parts(both)
        none = jnp.zeros((S, 2 * B), F32)
        ones = rows_of((1.0, 1.0, 1.0), 2 * B)
        pside[0] = jnp.concatenate([none, b1, b1, b1, ones, none[:32]], 0).astype(BF16)
        pside[1] = jnp.concatenate([none, b2, b2, none[:48]], 0).astype(BF16)
        pside[2] = jnp.concatenate([none, b3, none[:56]], 0).astype(BF16)
        prior_s[...] = jnp.zeros_like(prior_s)
        for t in range(half):
            two = jnp.concatenate([ptsi[2 * t], ptsi[2 * t + 1]], 1)
            right[t] = exponent_right(two).astype(BF16)
        got("pts_d", 0, ptsj.at[pl.ds(oc * np_, np_)])

    def kern_block(j, carry):
        two = jnp.concatenate([ptsj[2 * j], ptsj[2 * j + 1]], 1)
        left = exponent_left(two).T.astype(BF16)
        row = pl.multiple_of(j * 2 * B, 2 * B)
        for t in range(half):
            kern[t, pl.ds(row, 2 * B), :] = jnp.exp2(mm(left, right[t])).astype(BF16)
        return carry

    early = (np_ * KERN_EARLY) // 16
    with jax.named_scope("d_kern"):
        lax.fori_loop(0, early, kern_block, 0)

    with jax.named_scope("e_prior"):
        spans = sorted(range(nx), key=lambda d: hops(d, nx))
        for stage in range(2):
            columns = []
            for dx in spans:
                base = xs[(nx - dx) % nx] * ny
                group = bundle.at[stage, pl.ds(0, ny - 1)] if dx == 0 else bundle.at[stage, pl.ds(base, ny)]
                got("prm%d" % stage, dx, group)
                columns.append(base)
            for bases in (columns[:2], columns[2:]):
                pick = [(base + q, k) for k in range(2) for base in bases for q in range(ny)]
                part = jnp.concatenate([bundle[stage, slot, k] for slot, k in pick], 0)
                rest = jnp.concatenate([bundle[stage, base + q, 2] for base in bases for q in range(ny)], 0)
                cut = rest.shape[0]
                turns = mm(part, pside[0]) + mm(part, pside[1]) + mm(part, pside[2])
                feats = cos_turns(turns)
                f1 = feats.astype(BF16)
                f2 = (feats - f1.astype(F32)).astype(BF16)
                total = (mm(part, f1, flip) + mm(part, f2, flip))[:S]
                prior_s[...] += total + mm(rest, f1[:cut], flip)[:S] + mm(rest, f1[cut:], flip)[S:]

    with jax.named_scope("f_swap"):
        rcv[2, 1] = prior_s[:, B:]
        put("prior", 0, rcv.at[2, 1], rcv.at[2, 0], twin)
        sent("prior", rcv.at[2, 1])
        for copy in arrivals[4:]:
            copy.wait()
        got("prior", 0, rcv.at[2, 0])
        scale = math.sqrt(2.0 / nfeat)
        prior = scale * (prior_s[:, :B] + rcv[2, 0])
        rhs = tgt[...] - prior - 0.5 * noise[...]
        rhs_s[0] = prior
        rhs_s[1] = rhs
        low[0, c * np_ + p] = rhs.astype(BF16)
        low_z[0, z] = rhs.astype(BF16)

    def matvec(n, first, each, last):
        pn, dn, zn, on = "low%d_p" % n, "low%d_d" % n, "low%d_z" % n, "out%d" % n
        own = low.at[n, c * np_ + p]
        with jax.named_scope("g%d_send" % n):
            for d in far_p:
                put(pn, d // ny, own, own, plane_dev(d))
            for d in far_z:
                put(zn, 0, own, low_z.at[n, z], zdev(d, c))
            sent(pn, low.at[n, pl.ds(0, np_ - 1)])
            sent(zn, low_z.at[n, pl.ds(0, nz - 1)])
            sent(dn, low.at[n, pl.ds(0, np_)])
        with jax.named_scope("h%d_first" % n):
            first()

        def group_of(core, dx):
            return low.at[n, pl.ds(core * np_ + xs[(nx - dx) % nx] * ny, ny)]

        def own_group(dx):
            group = group_of(c, dx)
            got(pn, dx, low.at[n, pl.ds(0, ny - 1)] if dx == 0 else group)
            put(dn, dx, group, group, twin)

        def twin_group(dx):
            got(dn, dx, group_of(oc, dx))

        def times(core, dx, t):
            base = core * np_ + xs[(nx - dx) % nx] * ny
            fields = jnp.concatenate([low[n, base + q] for q in range(ny)], 1)
            row = pl.multiple_of(base * B, B * ny)
            return mm(fields, kern[t, pl.ds(row, B * ny), :])

        def add_tiles(groups, fresh):
            for t in range(half):
                out = times(*groups[0], t)
                for group in groups[1:]:
                    out = out + times(*group, t)
                for s in range(2):
                    piece = out[:, s * B:(s + 1) * B]
                    zz = 2 * t + s
                    outb[n, zz] = piece if fresh else outb[n, zz] + piece

        spans = sorted(range(nx), key=lambda d: hops(d, nx))
        with jax.named_scope("i%d_gather_a" % n):
            own_group(spans[0])
            own_group(spans[1])
        with jax.named_scope("i%d_gather_b" % n):
            add_tiles([(c, spans[0]), (c, spans[1])], True)
        with jax.named_scope("i%d_gather_c" % n):
            own_group(spans[2])
            own_group(spans[3])
            twin_group(spans[0])
        with jax.named_scope("i%d_gather_d" % n):
            add_tiles([(c, spans[2]), (c, spans[3]), (oc, spans[0])], False)
        with jax.named_scope("i%d_gather_e" % n):
            got(zn, 0, low_z.at[n, pl.ds(0, nz - 1)])
            twin_group(spans[1])
            twin_group(spans[2])
            twin_group(spans[3])
            flush()

        with jax.named_scope("j%d_tiles" % n):
            sums = None
            for t in range(half):
                out = times(oc, spans[1], t) + times(oc, spans[2], t) + times(oc, spans[3], t)
                for s in range(2):
                    zz = 2 * t + s
                    piece = outb[n, zz] + out[:, s * B:(s + 1) * B]
                    outb[n, zz] = piece
                    terms = each(zz, piece)
                    sums = terms if sums is None else [a + b for a, b in zip(sums, terms)]
            for d in far_z:
                put(on, 0, outb.at[n, zs[d]], rcv.at[n, z], zdev(d, c))
            sent(on, outb.at[n, pl.ds(0, nz - 1)])
        with jax.named_scope("k%d_last" % n):
            last(sums)
        with jax.named_scope("l%d_reduce" % n):
            total = outb[n, z]
            got(on, 0, rcv.at[n, pl.ds(0, nz - 1)])
            for d in near_z:
                total = total + rcv[n, zfrom(d)]
        return total

    def z_start(name, buf, value):
        zc = 2 * z + c
        buf[zc] = value
        for d in far_z:
            put(name + "_z", 0, buf.at[zc], buf.at[zc], zdev(d, c))
            put(name + "_z", 0, buf.at[zc], buf.at[zc], zdev(d, oc))
        put(name + "_z", 0, buf.at[zc], buf.at[zc], twin)
        sent(name + "_z", buf.at[pl.ds(0, 2 * nz - 1)])

    def z_end(name, buf):
        got(name + "_z", 0, buf.at[pl.ds(0, 2 * nz - 1)])
        return sum_all(buf, 2 * nz)

    def p_start(name, buf, value):
        buf[p] = value
        for d in far_p:
            put(name + "_p", 0, buf.at[p], buf.at[p], plane_dev(d))
        sent(name + "_p", buf.at[pl.ds(0, np_ - 1)])

    def p_end(name, buf):
        got(name + "_p", 0, buf.at[pl.ds(0, np_ - 1)])
        return sum_all(buf, np_)

    def sum_all(buf, count):
        parts = [buf[k] for k in range(count)]
        while len(parts) > 1:
            parts = [a + b for a, b in zip(parts[::2], parts[1::2])]
        return parts[0]

    def spread(row):
        return jnp.broadcast_to(row, (128, 128)).T

    def lane_sums(arrays):
        return jnp.sum(jnp.concatenate(arrays, 0).T, 0, keepdims=True)

    def first0():
        lax.fori_loop(early, np_, kern_block, 0)

    def each0(zz, piece):
        return [piece * low_z[0, zz].astype(F32)]

    def last0(sums):
        r = rhs_s[1]
        p_start("cur0", cur_p.at[0], lane_sums([*sums, r * r]))
        z_start("cur0", cur_z.at[0], p_end("cur0", cur_p.at[0]))

    k0 = matvec(0, first0, each0, last0)
    with jax.named_scope("m_alpha"):
        rhs = rhs_s[1]
        q1 = k0 + JITTER * rhs
        rhs_s[2] = k0
        sums = spread(z_end("cur0", cur_z.at[0]))
        m0 = sums[S:]
        alpha = m0 / (sums[:S] + JITTER * m0)
        r1 = rhs - alpha * q1
        low[1, c * np_ + p] = r1.astype(BF16)
        low_z[1, z] = r1.astype(BF16)
        rhs_s[3] = r1
        rhs_s[4] = alpha
        rhs_s[5] = m0

    def first1():
        r, k, new = rhs_s[1], rhs_s[2], rhs_s[3]
        sums = lane_sums([new * new, new * r, new * k, r * k])
        z_start("mom", mom_z, jnp.concatenate([sums[:, :128], sums[:, 128:]], 0))

    def each1(zz, piece):
        return [piece * low_z[1, zz].astype(F32), piece * low_z[0, zz].astype(F32)]

    def last1(sums):
        p_start("cur1", cur_p.at[1], lane_sums(sums))
        p_start("mom", mom_p, z_end("mom", mom_z))
        z_start("cur1", cur_z.at[1], p_end("cur1", cur_p.at[1]))

    k1 = matvec(1, first1, each1, last1)
    with jax.named_scope("n_finish"):
        prior, r, k0, r1, alpha, m0 = (rhs_s[k] for k in range(6))
        mom = p_end("mom", mom_p)
        one, two = spread(mom[0:1]), spread(mom[1:2])
        n1, r1r, r1k, rk = one[:S], one[S:], two[:S], two[S:]
        beta = n1 / m0
        kd = k1 + beta * k0
        dire = r1 + beta * r
        dd = n1 + beta * (2.0 * r1r + beta * m0)
        known = beta * (r1k + beta * rk) + JITTER * dd
        part = spread(z_end("cur1", cur_z.at[1]))
        alpha2 = n1 / (part[:S] + beta * part[S:] + known)
        out_ref[:S] = prior + alpha * k0 + alpha2 * kd
        out_ref[S:] = r1 - alpha2 * (kd + JITTER * dire)

        flush()

        @pl.when(mine)
        def _():
            whole = halves.at[pl.ds(0, nz - 1)]
            rdma("prm_z", 0, whole, whole, twin).wait_send()


def body(sizes, points, targets, noise, omega, phase, weights):
    nx, nz, ny = sizes
    np_, half = nx * ny, nz // 2
    vmem = pl.BlockSpec(memory_space=pltpu.VMEM)
    hbm = pl.BlockSpec(memory_space=pltpu.HBM)
    block = pltpu.VMEM((2 * S, B), F32)
    both = pl.pallas_call(
        functools.partial(kernel, sizes),
        out_shape=block,
        in_specs=[hbm] * 6,
        out_specs=vmem,
        scratch_shapes=[
            pltpu.VMEM((D, B), F32),
            pltpu.VMEM((1, B), F32),
            pltpu.VMEM((S, B), F32),
            pltpu.VMEM((D, FB), F32),
            pltpu.VMEM((1, FB), F32),
            pltpu.VMEM((FB, S), F32),
            pltpu.VMEM((2, FB, 128), BF16),
            pltpu.VMEM((2, np_, 3, FB, 128), BF16),
            pltpu.VMEM((D, B), F32),
            pltpu.VMEM((2 * np_, D, B), F32),
            pltpu.VMEM((nz, D, B), F32),
            pltpu.VMEM((3, 128, 2 * B), BF16),
            pltpu.VMEM((S, 2 * B), F32),
            pltpu.VMEM((nz, 2, FB, 128), BF16),
            pltpu.VMEM((6, S, B), F32),
            pltpu.VMEM((2, 2 * np_, S, B), BF16),
            pltpu.VMEM((2, nz, S, B), BF16),
            pltpu.VMEM((half, 64, 2 * B), BF16),
            pltpu.VMEM((half, 2 * np_ * B, 2 * B), BF16),
            pltpu.VMEM((2, nz, S, B), F32),
            pltpu.VMEM((3, nz, S, B), F32),
            pltpu.VMEM((2 * nz, 2, 128), F32),
            pltpu.VMEM((np_, 2, 128), F32),
            pltpu.VMEM((2, 2 * nz, 1, 128), F32),
            pltpu.VMEM((2, np_, 1, 128), F32),
            pltpu.SemaphoreType.DMA((len(SENDS()),)),
            pltpu.SemaphoreType.DMA((sum(count for _, count in RECVS(nx)),)),
            pltpu.SemaphoreType.DMA((6,)),
        ],
        compiler_params=pltpu.CompilerParams(
            collective_id=0, has_side_effects=True, vmem_limit_bytes=62000000),
    )(points, targets[None, :], noise, omega, phase[None, :], weights)
    return both[:S], both[S:]


def build(mesh, sizes):
    finer = Mesh(mesh.devices.reshape(*sizes, mesh.shape["cols"]), AXES)
    in_specs = (
        P(None, COLS_ROWS),
        P(COLS_ROWS),
        P(None, COLS_ROWS),
        P(None, ROWS),
        P(ROWS),
        P(ROWS, None),
    )
    out_specs = (P(None, COLS_ROWS), P(None, COLS_ROWS))
    return jax.shard_map(
        functools.partial(body, sizes), mesh=finer, in_specs=in_specs, out_specs=out_specs,
        check_vma=False)


def solution(mesh):
    return build(mesh, (4, 8, 4))
```

```python
import functools
import math

import jax
import jax.numpy as jnp
from jax import lax
from jax.experimental import pallas as pl
from jax.experimental.pallas import tpu as pltpu
from jax.sharding import Mesh
from jax.sharding import PartitionSpec as P

AXES = ("px", "pz", "py", "cols")
ROWS = ("px", "pz", "py")
COLS_ROWS = ("cols", "px", "pz", "py")
MESH = pl.DeviceIdType.MESH
F32, BF16 = jnp.float32, jnp.bfloat16

D = 8
S = 64
B = 128
FB = 16
JITTER = 0.25
KERN_EARLY = 6
SPREAD = math.sqrt(4.0 * math.log2(math.e))
SINE = [(-1) ** k * (2.0 * math.pi) ** (2 * k + 1) / math.factorial(2 * k + 1) for k in range(6)]


def SENDS():
    table = ["prm_z", "prm0", "prm1", "pts_z", "pts_p", "pts_d", "pts_o", "prior", "mom_z", "mom_p"]
    for n in "01":
        table += ["low%s_p" % n, "low%s_d" % n, "low%s_z" % n, "out%s" % n, "cur%s_z" % n, "cur%s_p" % n]
    return table


def RECVS(nx):
    several = {"prm_z": 4}
    for name in ("prm0", "prm1", "low0_p", "low0_d", "low1_p", "low1_d"):
        several[name] = nx
    return [(name, several.get(name, 1)) for name in SENDS()]


def three_parts(a):
    one = a.astype(BF16).astype(F32)
    rest = a - one
    two = rest.astype(BF16).astype(F32)
    three = (rest - two).astype(BF16).astype(F32)
    return one, two, three


def rows_of(pieces, width):
    row = lax.broadcasted_iota(jnp.int32, (8, width), 0)
    out = jnp.zeros((8, width), F32)
    for k, piece in enumerate(pieces):
        out = jnp.where(row == k, piece, out)
    return out


def exponent_left(points):
    scaled = points * SPREAD
    a1, a2, a3 = three_parts(scaled)
    n1, n2, n3 = three_parts(-0.5 * jnp.sum(scaled * scaled, 0, keepdims=True))
    width = points.shape[1]
    norms = rows_of((n1, n2, n3, 1.0, 1.0, 1.0), width)
    return jnp.concatenate([a1, a1, a2, a2, a1, a3, norms, jnp.zeros((8, width), F32)], 0)


def exponent_right(points):
    scaled = points * SPREAD
    b1, b2, b3 = three_parts(scaled)
    n1, n2, n3 = three_parts(-0.5 * jnp.sum(scaled * scaled, 0, keepdims=True))
    width = points.shape[1]
    norms = rows_of((1.0, 1.0, 1.0, n1, n2, n3), width)
    return jnp.concatenate([b1, b2, b1, b2, b3, b1, norms, jnp.zeros((8, width), F32)], 0)


def cos_turns(t):
    r = t - jnp.floor(t + 0.5)
    v = 0.25 - jnp.abs(r)
    w = v * v
    acc = jnp.full_like(w, SINE[-1])
    for c in SINE[-2::-1]:
        acc = acc * w + c
    return acc * v


def mm(a, b, dims=(((1,), (0,)), ((), ()))):
    return lax.dot_general(a, b, dims, preferred_element_type=F32)


def kernel(
    sizes,
    pts_hbm, tgt_hbm, noise_hbm, omega_hbm, phase_hbm, weights_hbm,
    out_ref,
    pts, tgt, noise, omega, phase, weights,
    prm_own, bundle, ptw, ptsj, ptsi, pside, prior_s, halves, rhs_s, low, low_z, right, kern, outb, rcv,
    mom_z, mom_p, cur_z, cur_p, mixes, send, recv, local,
):
    nx, nz, ny = sizes
    np_, half = nx * ny, nz // 2
    nfeat = nx * nz * ny * FB
    x, z, y, c = (lax.axis_index(a) for a in AXES)
    xs = [x] + [lax.rem(x + d, nx) for d in range(1, nx)]
    ys = [y] + [lax.rem(y + d, ny) for d in range(1, ny)]
    zs = [z] + [lax.rem(z + d, nz) for d in range(1, nz)]
    p = x * ny + y
    oc = 1 - c
    twin = (x, z, y, oc)

    arrivals = []
    for k, (src, dst) in enumerate((
        (weights_hbm, weights), (omega_hbm, omega), (phase_hbm, phase), (pts_hbm, pts),
        (tgt_hbm, tgt), (noise_hbm, noise),
    )):
        copy = pltpu.make_async_copy(src, dst, local.at[k])
        copy.start()
        arrivals.append(copy)

    at = {}
    top = 0
    for name, count in RECVS(nx):
        at[name] = top
        top += count
    order = {name: k for k, name in enumerate(SENDS())}

    def rdma(name, k, src, dst, dev):
        return pltpu.make_async_remote_copy(
            src_ref=src, dst_ref=dst, send_sem=send.at[order[name]], recv_sem=recv.at[at[name] + k],
            device_id=dev, device_id_type=MESH)

    pending = []

    def put(name, k, src, dst, dev):
        rdma(name, k, src, dst, dev).start()

    def sent(name, whole):
        pending.append((name, whole))

    def flush():
        for name, whole in pending:
            rdma(name, 0, whole, whole, twin).wait_send()
        pending.clear()

    def got(name, k, dst):
        rdma(name, k, dst, dst, twin).wait_recv()

    def hops(d, n):
        return min(d, n - d)

    def dxy(d):
        return d // ny, d % ny

    near_p = sorted(range(1, np_), key=lambda d: hops(d // ny, nx) + hops(d % ny, ny))
    far_p = near_p[::-1]
    near_z = sorted(range(1, nz), key=lambda d: hops(d, nz))
    far_z = near_z[::-1]

    def plane_dev(d, core=c):
        dx, dy = dxy(d)
        return (xs[dx], z, ys[dy], core)

    def plane_slot(d):
        dx, dy = dxy(d)
        return xs[(nx - dx) % nx] * ny + ys[(ny - dy) % ny]

    def zdev(d, core):
        return (x, zs[d], y, core)

    def zfrom(d):
        return zs[(nz - d) % nz]

    with jax.named_scope("a_barrier"):
        bar = pltpu.get_barrier_semaphore()

        def greet(dev):
            pl.semaphore_signal(bar, inc=1, device_id=dev, device_id_type=MESH)

        for d in far_p:
            greet(plane_dev(d))
            greet(plane_dev(d, oc))
        for d in far_z:
            greet(zdev(d, c))
        greet(twin)

        turn = 1.0 / (2.0 * math.pi)
        for copy in arrivals[:4]:
            copy.wait()
        lane = lax.broadcasted_iota(jnp.int32, (FB, 128), 1)
        row = lax.broadcasted_iota(jnp.int32, (FB, 128), 0)
        angles = jnp.concatenate([omega[...], phase[...], jnp.zeros((FB - D - 1, FB), F32)], 0) * turn
        packed = jnp.zeros((FB, 128), F32)
        flip = (((0,), (0,)), ((), ()))
        for k, piece in enumerate(three_parts(angles)):
            spot = jnp.where(row < D, S + k * D + row, S + 3 * D + k)
            pick = jnp.where((lane == spot) & (row <= D), 1.0, 0.0)
            packed = packed + mm(piece.astype(BF16), pick.astype(BF16), flip)
        w1 = weights[...].astype(BF16)
        w2 = (weights[...] - w1.astype(F32)).astype(BF16)
        wide = lax.broadcasted_iota(jnp.int32, (S, 128), 1)
        deep = lax.broadcasted_iota(jnp.int32, (S, 128), 0)
        once = jnp.where(wide == deep, 1.0, 0.0).astype(BF16)
        twice = jnp.where((wide == deep) | (wide == deep + S), 1.0, 0.0).astype(BF16)
        prm_own[0] = (packed + mm(w1, once)).astype(BF16)
        prm_own[1] = mm(w2, twice).astype(BF16)
        pl.semaphore_wait(bar, 1 + (nz - 1) + 2 * (np_ - 1))

    mine = lax.rem(z, 2) == c
    zslot = lax.div(z, 2)

    with jax.named_scope("b_prm_z"):
        par = lax.rem(z + c, 2)
        turnout = {1: 0, 7: 1, 3: 2, 5: 3, 2: 1, 6: 2, 4: 3}
        places = [par, 2 + 5 * par, 6 - 3 * par, 4 + par]

        @pl.when(mine)
        def _():
            for d in far_z:
                put("prm_z", turnout[d], prm_own, halves.at[d], zdev(d, c))
            halves[0] = prm_own[...]

        put("pts_o", 0, pts, ptw, twin)
        sent("pts_o", pts)
        for d in far_p:
            put("pts_p", 0, pts, ptsj.at[c * np_ + p], plane_dev(d))
        for d in far_z:
            put("pts_z", 0, pts, ptsi.at[z], zdev(d, c))
        sent("pts_p", ptsj.at[pl.ds(0, np_ - 1)])
        sent("pts_z", ptsi.at[pl.ds(0, nz - 1)])
        ptsj[c * np_ + p] = pts[...]
        ptsi[z] = pts[...]

        left_lanes = lax.broadcasted_iota(jnp.int32, (FB, 128), 1) < S
        for stage in range(2):
            if stage == 0:
                @pl.when(jnp.logical_not(mine))
                def _():
                    got("prm_z", 0, halves.at[1])
            else:
                got("prm_z", 2, halves.at[places[2]])
            got("prm_z", 2 * stage + 1, halves.at[places[2 * stage + 1]])
            one, two = halves[places[2 * stage]], halves[places[2 * stage + 1]]
            bundle[stage, p, 0] = one[0]
            bundle[stage, p, 1] = two[0]
            bundle[stage, p, 2] = jnp.where(left_lanes, one[1].astype(F32), two[1].astype(F32)).astype(BF16)
            name = "prm%d" % stage
            for d in far_p:
                put(name, d // ny, bundle.at[stage, p], bundle.at[stage, p], plane_dev(d))
            sent(name, bundle.at[stage, pl.ds(0, np_ - 1)])

    with jax.named_scope("c_points"):
        got("pts_o", 0, ptw)
        got("pts_p", 0, ptsj.at[pl.ds(0, np_ - 1)])
        here = ptsj.at[pl.ds(c * np_, np_)]
        put("pts_d", 0, here, here, twin)
        sent("pts_d", here)
        got("pts_z", 0, ptsi.at[pl.ds(0, nz - 1)])
        both = jnp.concatenate([pts[...], ptw[...]], 1)
        b1, b2, b3 = three_parts(both)
        none = jnp.zeros((S, 2 * B), F32)
        ones = rows_of((1.0, 1.0, 1.0), 2 * B)
        pside[0] = jnp.concatenate([none, b1, b1, b1, ones, none[:32]], 0).astype(BF16)
        pside[1] = jnp.concatenate([none, b2, b2, none[:48]], 0).astype(BF16)
        pside[2] = jnp.concatenate([none, b3, none[:56]], 0).astype(BF16)
        for t in range(half):
            two = jnp.concatenate([ptsi[2 * t], ptsi[2 * t + 1]], 1)
            right[t] = exponent_right(two).astype(BF16)
        got("pts_d", 0, ptsj.at[pl.ds(oc * np_, np_)])

    def kern_block(j, carry):
        two = jnp.concatenate([ptsj[2 * j], ptsj[2 * j + 1]], 1)
        left = exponent_left(two).T.astype(BF16)
        row = pl.multiple_of(j * 2 * B, 2 * B)
        for t in range(half):
            kern[t, pl.ds(row, 2 * B), :] = jnp.exp2(mm(left, right[t])).astype(BF16)
        return carry

    early = (np_ * KERN_EARLY) // 16
    with jax.named_scope("d_kern"):
        lax.fori_loop(0, early, kern_block, 0)

    with jax.named_scope("e_prior"):
        spans = sorted(range(nx), key=lambda d: hops(d, nx))
        for stage in range(2):
            columns = []

            def columns_in(some):
                for dx in some:
                    base = xs[(nx - dx) % nx] * ny
                    group = bundle.at[stage, pl.ds(0, ny - 1)] if dx == 0 else bundle.at[stage, pl.ds(base, ny)]
                    got("prm%d" % stage, dx, group)
                    columns.append(base)

            columns_in(spans)

            def features(bases, lanes):
                pick = [(base + q, k) for k in range(2) for base in bases for q in range(ny)]
                part = jnp.concatenate([bundle[stage, slot, k] for slot, k in pick], 0)
                rest = jnp.concatenate([bundle[stage, base + q, 2] for base in bases for q in range(ny)], 0)
                cut = rest.shape[0]
                turns = mm(part, pside[0, :, lanes]) + mm(part, pside[1, :, lanes]) + mm(part, pside[2, :, lanes])
                feats = cos_turns(turns)
                f1 = feats.astype(BF16)
                f2 = (feats - f1.astype(F32)).astype(BF16)
                total = (mm(part, f1, flip) + mm(part, f2, flip))[:S]
                return total + mm(rest, f1[:cut], flip)[:S] + mm(rest, f1[cut:], flip)[S:]

            couples = (columns[:2], columns[2:])
            if stage == 0:
                prior_s[...] = sum(features(bases, slice(0, 2 * B)) for bases in couples)
            else:
                rcv[2, 1] = prior_s[:, B:] + sum(features(bases, slice(B, 2 * B)) for bases in couples)
                put("prior", 0, rcv.at[2, 1], rcv.at[2, 0], twin)
                sent("prior", rcv.at[2, 1])
                prior_own = prior_s[:, :B] + sum(features(bases, slice(0, B)) for bases in couples)

    with jax.named_scope("f_swap"):
        for copy in arrivals[4:]:
            copy.wait()
        got("prior", 0, rcv.at[2, 0])
        scale = math.sqrt(2.0 / nfeat)
        prior = scale * (prior_own + rcv[2, 0])
        rhs = tgt[...] - prior - 0.5 * noise[...]
        rhs_s[0] = prior
        rhs_s[1] = rhs
        low[0, c * np_ + p] = rhs.astype(BF16)
        low_z[0, z] = rhs.astype(BF16)

    def matvec(n, first, blend, each, last):
        pn, dn, zn, on = "low%d_p" % n, "low%d_d" % n, "low%d_z" % n, "out%d" % n
        own = low.at[n, c * np_ + p]
        with jax.named_scope("g%d_send" % n):
            for d in far_p:
                put(pn, d // ny, own, own, plane_dev(d))
            for d in far_z:
                put(zn, 0, own, low_z.at[n, z], zdev(d, c))
            sent(pn, low.at[n, pl.ds(0, np_ - 1)])
            sent(zn, low_z.at[n, pl.ds(0, nz - 1)])
            sent(dn, low.at[n, pl.ds(0, np_)])
        with jax.named_scope("h%d_first" % n):
            first()

        def group_of(core, dx):
            return low.at[n, pl.ds(core * np_ + xs[(nx - dx) % nx] * ny, ny)]

        def own_group(dx):
            group = group_of(c, dx)
            got(pn, dx, low.at[n, pl.ds(0, ny - 1)] if dx == 0 else group)
            put(dn, dx, group, group, twin)

        def twin_group(dx):
            got(dn, dx, group_of(oc, dx))

        def times(core, dx, t):
            base = core * np_ + xs[(nx - dx) % nx] * ny
            fields = jnp.concatenate([low[n, base + q] for q in range(ny)], 1)
            row = pl.multiple_of(base * B, B * ny)
            return mm(fields, kern[t, pl.ds(row, B * ny), :])

        def add_tiles(groups, fresh):
            for t in range(half):
                out = times(*groups[0], t)
                for group in groups[1:]:
                    out = out + times(*group, t)
                for s in range(2):
                    piece = out[:, s * B:(s + 1) * B]
                    zz = 2 * t + s
                    outb[n, zz] = piece if fresh else outb[n, zz] + piece

        spans = sorted(range(nx), key=lambda d: hops(d, nx))
        with jax.named_scope("i%d_gather_a" % n):
            for dx in spans:
                own_group(dx)
        with jax.named_scope("i%d_gather_b" % n):
            add_tiles([(c, dx) for dx in spans], True)
            flush()
        with jax.named_scope("i%d_gather_e" % n):
            got(zn, 0, low_z.at[n, pl.ds(0, nz - 1)])
            for dx in spans:
                twin_group(dx)

        with jax.named_scope("j%d_tiles" % n):
            sums = None
            for t in range(half):
                out = times(oc, spans[0], t)
                for dx in spans[1:]:
                    out = out + times(oc, dx, t)
                for s in range(2):
                    zz = 2 * t + s
                    piece = blend(zz, outb[n, zz] + out[:, s * B:(s + 1) * B])
                    outb[n, zz] = piece
                    terms = each(zz, piece)
                    sums = terms if sums is None else [a + b for a, b in zip(sums, terms)]
            for d in far_z:
                put(on, 0, outb.at[n, zs[d]], rcv.at[n, z], zdev(d, c))
            sent(on, outb.at[n, pl.ds(0, nz - 1)])
        with jax.named_scope("k%d_last" % n):
            last(sums)
        with jax.named_scope("l%d_reduce" % n):
            total = outb[n, z]
            got(on, 0, rcv.at[n, pl.ds(0, nz - 1)])
            for d in near_z:
                total = total + rcv[n, zfrom(d)]
        return total

    def z_start(name, buf, value):
        buf[z] = value
        for d in far_z:
            put(name + "_z", 0, buf.at[z], buf.at[z], zdev(d, c))
        sent(name + "_z", buf.at[pl.ds(0, nz - 1)])

    def z_end(name, buf):
        got(name + "_z", 0, buf.at[pl.ds(0, nz - 1)])
        return sum_all(buf, nz)

    def p_start(name, buf, value):
        slot = c * np_ + p
        buf[slot] = value
        for d in far_p:
            put(name + "_p", 0, buf.at[slot], buf.at[slot], plane_dev(d, oc))
            put(name + "_p", 0, buf.at[slot], buf.at[slot], plane_dev(d))
        put(name + "_p", 0, buf.at[slot], buf.at[slot], twin)
        sent(name + "_p", buf.at[pl.ds(0, 2 * np_ - 1)])

    def p_end(name, buf):
        got(name + "_p", 0, buf.at[pl.ds(0, 2 * np_ - 1)])
        return sum_all(buf, 2 * np_)

    def sum_all(buf, count):
        parts = [buf[k] for k in range(count)]
        while len(parts) > 1:
            parts = [a + b for a, b in zip(parts[::2], parts[1::2])]
        return parts[0]

    def spread(row):
        return jnp.broadcast_to(row, (128, 128)).T

    def lane_sums(arrays):
        return jnp.sum(jnp.concatenate(arrays, 0).T, 0, keepdims=True)

    def first0():
        lax.fori_loop(early, np_, kern_block, 0)

    def each0(zz, piece):
        return [piece * low_z[0, zz].astype(F32)]

    def blend0(zz, piece):
        return piece

    def near_alpha(row):
        both = spread(row)
        dot, norm = jnp.maximum(both[:S], 0.0), both[S:]
        return jnp.where(norm > 0.0, norm, 1.0) / jnp.where(norm > 0.0, dot + JITTER * norm, 1.0)

    def last0(sums):
        r = rhs_s[1]
        p_start("cur0", cur_p.at[0], lane_sums([*sums, r * r]))
        row = p_end("cur0", cur_p.at[0])
        z_start("cur0", cur_z.at[0], row)
        rhs_s[4] = near_alpha(row)

    k0 = matvec(0, first0, blend0, each0, last0)
    with jax.named_scope("m_alpha"):
        rhs = rhs_s[1]
        q1 = k0 + JITTER * rhs
        rhs_s[2] = k0
        basis = rhs - rhs_s[4] * q1
        low[1, c * np_ + p] = basis.astype(BF16)
        low_z[1, z] = basis.astype(BF16)
        rhs_s[3] = q1

    def first1():
        r, k, q1 = rhs_s[1], rhs_s[2], rhs_s[3]
        sums = spread(z_end("cur0", cur_z.at[0]))
        m0 = sums[S:]
        alpha = m0 / (sums[:S] + JITTER * m0)
        new = r - alpha * q1
        rhs_s[3] = new
        rhs_s[4] = alpha
        rhs_s[5] = m0
        sums = lane_sums([new * new, new * r, new * k, r * k])
        z_start("mom", mom_z, jnp.concatenate([sums[:, :128], sums[:, 128:]], 0))
        for zz in range(nz):
            mixes[zz] = alpha / near_alpha(cur_z[0, zz])

    def blend1(zz, piece):
        mix = mixes[z]
        return mix * piece + (1.0 - mix) * outb[0, zz]

    def each1(zz, piece):
        mix, r = mixes[zz], low_z[0, zz].astype(F32)
        return [piece * (mix * low_z[1, zz].astype(F32) + (1.0 - mix) * r), piece * r]

    def last1(sums):
        p_start("cur1", cur_p.at[1], lane_sums(sums))
        p_start("mom", mom_p, z_end("mom", mom_z))
        z_start("cur1", cur_z.at[1], p_end("cur1", cur_p.at[1]))

    k1 = matvec(1, first1, blend1, each1, last1)
    with jax.named_scope("n_finish"):
        prior, r, k0, r1, alpha, m0 = (rhs_s[k] for k in range(6))
        mom = p_end("mom", mom_p)
        one, two = spread(mom[0:1]), spread(mom[1:2])
        n1, r1r, r1k, rk = one[:S], one[S:], two[:S], two[S:]
        beta = n1 / m0
        kd = k1 + beta * k0
        dire = r1 + beta * r
        dd = n1 + beta * (2.0 * r1r + beta * m0)
        known = beta * (r1k + beta * rk) + JITTER * dd
        part = spread(z_end("cur1", cur_z.at[1]))
        alpha2 = n1 / (part[:S] + beta * part[S:] + known)
        out_ref[:S] = prior + alpha * k0 + alpha2 * kd
        out_ref[S:] = r1 - alpha2 * (kd + JITTER * dire)

        flush()

        @pl.when(mine)
        def _():
            whole = halves.at[pl.ds(0, nz - 1)]
            rdma("prm_z", 0, whole, whole, twin).wait_send()


def body(sizes, points, targets, noise, omega, phase, weights):
    nx, nz, ny = sizes
    np_, half = nx * ny, nz // 2
    vmem = pl.BlockSpec(memory_space=pltpu.VMEM)
    hbm = pl.BlockSpec(memory_space=pltpu.HBM)
    block = pltpu.VMEM((2 * S, B), F32)
    both = pl.pallas_call(
        functools.partial(kernel, sizes),
        out_shape=block,
        in_specs=[hbm] * 6,
        out_specs=vmem,
        scratch_shapes=[
            pltpu.VMEM((D, B), F32),
            pltpu.VMEM((1, B), F32),
            pltpu.VMEM((S, B), F32),
            pltpu.VMEM((D, FB), F32),
            pltpu.VMEM((1, FB), F32),
            pltpu.VMEM((FB, S), F32),
            pltpu.VMEM((2, FB, 128), BF16),
            pltpu.VMEM((2, np_, 3, FB, 128), BF16),
            pltpu.VMEM((D, B), F32),
            pltpu.VMEM((2 * np_, D, B), F32),
            pltpu.VMEM((nz, D, B), F32),
            pltpu.VMEM((3, 128, 2 * B), BF16),
            pltpu.VMEM((S, 2 * B), F32),
            pltpu.VMEM((nz, 2, FB, 128), BF16),
            pltpu.VMEM((6, S, B), F32),
            pltpu.VMEM((2, 2 * np_, S, B), BF16),
            pltpu.VMEM((2, nz, S, B), BF16),
            pltpu.VMEM((half, 64, 2 * B), BF16),
            pltpu.VMEM((half, 2 * np_ * B, 2 * B), BF16),
            pltpu.VMEM((2, nz, S, B), F32),
            pltpu.VMEM((3, nz, S, B), F32),
            pltpu.VMEM((nz, 2, 128), F32),
            pltpu.VMEM((2 * np_, 2, 128), F32),
            pltpu.VMEM((2, nz, 1, 128), F32),
            pltpu.VMEM((2, 2 * np_, 1, 128), F32),
            pltpu.VMEM((nz, S, B), F32),
            pltpu.SemaphoreType.DMA((len(SENDS()),)),
            pltpu.SemaphoreType.DMA((sum(count for _, count in RECVS(nx)),)),
            pltpu.SemaphoreType.DMA((6,)),
        ],
        compiler_params=pltpu.CompilerParams(
            collective_id=0, has_side_effects=True, vmem_limit_bytes=62000000),
    )(points, targets[None, :], noise, omega, phase[None, :], weights)
    return both[:S], both[S:]


def build(mesh, sizes):
    finer = Mesh(mesh.devices.reshape(*sizes, mesh.shape["cols"]), AXES)
    in_specs = (
        P(None, COLS_ROWS),
        P(COLS_ROWS),
        P(None, COLS_ROWS),
        P(None, ROWS),
        P(ROWS),
        P(ROWS, None),
    )
    out_specs = (P(None, COLS_ROWS), P(None, COLS_ROWS))
    return jax.shard_map(
        functools.partial(body, sizes), mesh=finer, in_specs=in_specs, out_specs=out_specs,
        check_vma=False)


def solution(mesh):
    return build(mesh, (4, 8, 4))
```

```python
import functools
import math

import jax
import jax.numpy as jnp
from jax import lax
from jax.experimental import pallas as pl
from jax.experimental.pallas import tpu as pltpu
from jax.sharding import Mesh
from jax.sharding import PartitionSpec as P

AXES = ("px", "pz", "py", "cols")
ROWS = ("px", "pz", "py")
COLS_ROWS = ("cols", "px", "pz", "py")
MESH = pl.DeviceIdType.MESH
F32, BF16 = jnp.float32, jnp.bfloat16

D = 8
S = 64
B = 128
FB = 16
JITTER = 0.25
KERN_EARLY = 8
SPREAD = math.sqrt(4.0 * math.log2(math.e))
SINE = [(-1) ** k * (2.0 * math.pi) ** (2 * k + 1) / math.factorial(2 * k + 1) for k in range(6)]


def SENDS():
    table = ["prm_z", "prm0", "prm1", "pts_z", "pts_p", "pts_d", "pts_o", "prior", "mom_z", "mom_p"]
    for n in "01":
        table += ["low%s_p" % n, "low%s_d" % n, "low%s_z" % n, "out%s" % n, "cur%s_z" % n, "cur%s_p" % n]
    return table


def RECVS(nx):
    several = {"prm_z": 4}
    for name in ("prm0", "prm1", "low0_p", "low0_d", "low1_p", "low1_d"):
        several[name] = nx
    return [(name, several.get(name, 1)) for name in SENDS()]


def three_parts(a):
    one = a.astype(BF16).astype(F32)
    rest = a - one
    two = rest.astype(BF16).astype(F32)
    three = (rest - two).astype(BF16).astype(F32)
    return one, two, three


def rows_of(pieces, width):
    row = lax.broadcasted_iota(jnp.int32, (8, width), 0)
    out = jnp.zeros((8, width), F32)
    for k, piece in enumerate(pieces):
        out = jnp.where(row == k, piece, out)
    return out


def exponent_left(points):
    scaled = points * SPREAD
    a1, a2, a3 = three_parts(scaled)
    n1, n2, n3 = three_parts(-0.5 * jnp.sum(scaled * scaled, 0, keepdims=True))
    width = points.shape[1]
    norms = rows_of((n1, n2, n3, 1.0, 1.0, 1.0), width)
    return jnp.concatenate([a1, a1, a2, a2, a1, a3, norms, jnp.zeros((8, width), F32)], 0)


def exponent_right(points):
    scaled = points * SPREAD
    b1, b2, b3 = three_parts(scaled)
    n1, n2, n3 = three_parts(-0.5 * jnp.sum(scaled * scaled, 0, keepdims=True))
    width = points.shape[1]
    norms = rows_of((1.0, 1.0, 1.0, n1, n2, n3), width)
    return jnp.concatenate([b1, b2, b1, b2, b3, b1, norms, jnp.zeros((8, width), F32)], 0)


def cos_turns(t):
    r = t - jnp.floor(t + 0.5)
    v = 0.25 - jnp.abs(r)
    w = v * v
    acc = jnp.full_like(w, SINE[-1])
    for c in SINE[-2::-1]:
        acc = acc * w + c
    return acc * v


def mm(a, b, dims=(((1,), (0,)), ((), ()))):
    return lax.dot_general(a, b, dims, preferred_element_type=F32)


def kernel(
    sizes,
    pts_hbm, tgt_hbm, noise_hbm, omega_hbm, phase_hbm, weights_hbm,
    out_ref,
    pts, tgt, noise, omega, phase, weights,
    prm_own, bundle, ptw, ptsj, ptsi, pside, prior_s, halves, rhs_s, low, low_z, right, kern, outb, rcv,
    mom_z, mom_p, cur_z, cur_p, mixes, send, recv, local,
):
    nx, nz, ny = sizes
    np_, half = nx * ny, nz // 2
    nfeat = nx * nz * ny * FB
    x, z, y, c = (lax.axis_index(a) for a in AXES)
    xs = [x] + [lax.rem(x + d, nx) for d in range(1, nx)]
    ys = [y] + [lax.rem(y + d, ny) for d in range(1, ny)]
    zs = [z] + [lax.rem(z + d, nz) for d in range(1, nz)]
    p = x * ny + y
    oc = 1 - c
    twin = (x, z, y, oc)

    arrivals = []
    for k, (src, dst) in enumerate((
        (weights_hbm, weights), (omega_hbm, omega), (phase_hbm, phase), (pts_hbm, pts),
        (tgt_hbm, tgt), (noise_hbm, noise),
    )):
        copy = pltpu.make_async_copy(src, dst, local.at[k])
        copy.start()
        arrivals.append(copy)

    at = {}
    top = 0
    for name, count in RECVS(nx):
        at[name] = top
        top += count
    order = {name: k for k, name in enumerate(SENDS())}

    def rdma(name, k, src, dst, dev):
        return pltpu.make_async_remote_copy(
            src_ref=src, dst_ref=dst, send_sem=send.at[order[name]], recv_sem=recv.at[at[name] + k],
            device_id=dev, device_id_type=MESH)

    pending = []

    def put(name, k, src, dst, dev):
        rdma(name, k, src, dst, dev).start()

    def sent(name, whole):
        pending.append((name, whole))

    def flush():
        for name, whole in pending:
            rdma(name, 0, whole, whole, twin).wait_send()
        pending.clear()

    def got(name, k, dst):
        rdma(name, k, dst, dst, twin).wait_recv()

    def hops(d, n):
        return min(d, n - d)

    def dxy(d):
        return d // ny, d % ny

    near_p = sorted(range(1, np_), key=lambda d: hops(d // ny, nx) + hops(d % ny, ny))
    far_p = near_p[::-1]
    near_z = sorted(range(1, nz), key=lambda d: hops(d, nz))
    far_z = near_z[::-1]

    def plane_dev(d, core=c):
        dx, dy = dxy(d)
        return (xs[dx], z, ys[dy], core)

    def plane_slot(d):
        dx, dy = dxy(d)
        return xs[(nx - dx) % nx] * ny + ys[(ny - dy) % ny]

    def zdev(d, core):
        return (x, zs[d], y, core)

    def zfrom(d):
        return zs[(nz - d) % nz]

    with jax.named_scope("a_barrier"):
        bar = pltpu.get_barrier_semaphore()

        def greet(dev):
            pl.semaphore_signal(bar, inc=1, device_id=dev, device_id_type=MESH)

        for d in far_p:
            greet(plane_dev(d))
            greet(plane_dev(d, oc))
        for d in far_z:
            greet(zdev(d, c))
        greet(twin)

        turn = 1.0 / (2.0 * math.pi)
        for copy in arrivals[:4]:
            copy.wait()
        lane = lax.broadcasted_iota(jnp.int32, (FB, 128), 1)
        row = lax.broadcasted_iota(jnp.int32, (FB, 128), 0)
        angles = jnp.concatenate([omega[...], phase[...], jnp.zeros((FB - D - 1, FB), F32)], 0) * turn
        packed = jnp.zeros((FB, 128), F32)
        flip = (((0,), (0,)), ((), ()))
        for k, piece in enumerate(three_parts(angles)):
            spot = jnp.where(row < D, S + k * D + row, S + 3 * D + k)
            pick = jnp.where((lane == spot) & (row <= D), 1.0, 0.0)
            packed = packed + mm(piece.astype(BF16), pick.astype(BF16), flip)
        w1 = weights[...].astype(BF16)
        w2 = (weights[...] - w1.astype(F32)).astype(BF16)
        wide = lax.broadcasted_iota(jnp.int32, (S, 128), 1)
        deep = lax.broadcasted_iota(jnp.int32, (S, 128), 0)
        once = jnp.where(wide == deep, 1.0, 0.0).astype(BF16)
        twice = jnp.where((wide == deep) | (wide == deep + S), 1.0, 0.0).astype(BF16)
        prm_own[0] = (packed + mm(w1, once)).astype(BF16)
        prm_own[1] = mm(w2, twice).astype(BF16)
        pl.semaphore_wait(bar, 1 + (nz - 1) + 2 * (np_ - 1))

    mine = lax.rem(z, 2) == c
    zslot = lax.div(z, 2)

    with jax.named_scope("b_prm_z"):
        par = lax.rem(z + c, 2)
        turnout = {1: 0, 7: 1, 3: 2, 5: 3, 2: 1, 6: 2, 4: 3}
        places = [par, 2 + 5 * par, 6 - 3 * par, 4 + par]

        @pl.when(mine)
        def _():
            for d in far_z:
                put("prm_z", turnout[d], prm_own, halves.at[d], zdev(d, c))
            halves[0] = prm_own[...]

        put("pts_o", 0, pts, ptw, twin)
        sent("pts_o", pts)
        for d in far_p:
            put("pts_p", 0, pts, ptsj.at[c * np_ + p], plane_dev(d))
        for d in far_z:
            put("pts_z", 0, pts, ptsi.at[z], zdev(d, c))
        sent("pts_p", ptsj.at[pl.ds(0, np_ - 1)])
        sent("pts_z", ptsi.at[pl.ds(0, nz - 1)])
        ptsj[c * np_ + p] = pts[...]
        ptsi[z] = pts[...]

        left_lanes = lax.broadcasted_iota(jnp.int32, (FB, 128), 1) < S
        for stage in range(2):
            if stage == 0:
                @pl.when(jnp.logical_not(mine))
                def _():
                    got("prm_z", 0, halves.at[1])
            else:
                got("prm_z", 2, halves.at[places[2]])
            got("prm_z", 2 * stage + 1, halves.at[places[2 * stage + 1]])
            one, two = halves[places[2 * stage]], halves[places[2 * stage + 1]]
            bundle[stage, p, 0] = one[0]
            bundle[stage, p, 1] = two[0]
            bundle[stage, p, 2] = jnp.where(left_lanes, one[1].astype(F32), two[1].astype(F32)).astype(BF16)
            name = "prm%d" % stage
            for d in far_p:
                put(name, d // ny, bundle.at[stage, p], bundle.at[stage, p], plane_dev(d))
            sent(name, bundle.at[stage, pl.ds(0, np_ - 1)])

    with jax.named_scope("c_points"):
        got("pts_o", 0, ptw)
        got("pts_p", 0, ptsj.at[pl.ds(0, np_ - 1)])
        here = ptsj.at[pl.ds(c * np_, np_)]
        put("pts_d", 0, here, here, twin)
        sent("pts_d", here)
        got("pts_z", 0, ptsi.at[pl.ds(0, nz - 1)])
        both = jnp.concatenate([pts[...], ptw[...]], 1)
        b1, b2, b3 = three_parts(both)
        none = jnp.zeros((S, 2 * B), F32)
        ones = rows_of((1.0, 1.0, 1.0), 2 * B)
        pside[0] = jnp.concatenate([none, b1, b1, b1, ones, none[:32]], 0).astype(BF16)
        pside[1] = jnp.concatenate([none, b2, b2, none[:48]], 0).astype(BF16)
        pside[2] = jnp.concatenate([none, b3, none[:56]], 0).astype(BF16)
        for t in range(half):
            two = jnp.concatenate([ptsi[2 * t], ptsi[2 * t + 1]], 1)
            right[t] = exponent_right(two).astype(BF16)
        got("pts_d", 0, ptsj.at[pl.ds(oc * np_, np_)])

    def kern_block(j, carry):
        two = jnp.concatenate([ptsj[2 * j], ptsj[2 * j + 1]], 1)
        left = exponent_left(two).T.astype(BF16)
        row = pl.multiple_of(j * 2 * B, 2 * B)
        for t in range(half):
            kern[t, pl.ds(row, 2 * B), :] = jnp.exp2(mm(left, right[t])).astype(BF16)
        return carry

    early = (np_ * KERN_EARLY) // 16
    with jax.named_scope("d_kern"):
        lax.fori_loop(0, early, kern_block, 0)

    with jax.named_scope("e_prior"):
        spans = sorted(range(nx), key=lambda d: hops(d, nx))
        for stage in range(2):
            columns = []

            def columns_in(some):
                for dx in some:
                    base = xs[(nx - dx) % nx] * ny
                    group = bundle.at[stage, pl.ds(0, ny - 1)] if dx == 0 else bundle.at[stage, pl.ds(base, ny)]
                    got("prm%d" % stage, dx, group)
                    columns.append(base)

            columns_in(spans)

            def features(bases, lanes):
                pick = [(base + q, k) for k in range(2) for base in bases for q in range(ny)]
                part = jnp.concatenate([bundle[stage, slot, k] for slot, k in pick], 0)
                rest = jnp.concatenate([bundle[stage, base + q, 2] for base in bases for q in range(ny)], 0)
                cut = rest.shape[0]
                turns = mm(part, pside[0, :, lanes]) + mm(part, pside[1, :, lanes]) + mm(part, pside[2, :, lanes])
                feats = cos_turns(turns)
                f1 = feats.astype(BF16)
                f2 = (feats - f1.astype(F32)).astype(BF16)
                total = (mm(part, f1, flip) + mm(part, f2, flip))[:S]
                return total + mm(rest, f1[:cut], flip)[:S] + mm(rest, f1[cut:], flip)[S:]

            couples = (columns[:2], columns[2:])
            if stage == 0:
                prior_s[...] = sum(features(bases, slice(0, 2 * B)) for bases in couples)
            else:
                rcv[2, 1] = prior_s[:, B:] + sum(features(bases, slice(B, 2 * B)) for bases in couples)
                put("prior", 0, rcv.at[2, 1], rcv.at[2, 0], twin)
                sent("prior", rcv.at[2, 1])
                prior_own = prior_s[:, :B] + sum(features(bases, slice(0, B)) for bases in couples)

    with jax.named_scope("f_swap"):
        for copy in arrivals[4:]:
            copy.wait()
        got("prior", 0, rcv.at[2, 0])
        scale = math.sqrt(2.0 / nfeat)
        prior = scale * (prior_own + rcv[2, 0])
        rhs = tgt[...] - prior - 0.5 * noise[...]
        rhs_s[0] = prior
        rhs_s[1] = rhs
        low[0, c * np_ + p] = rhs.astype(BF16)
        low_z[0, z] = rhs.astype(BF16)

    def matvec(n, first, blend, each, last):
        pn, dn, zn, on = "low%d_p" % n, "low%d_d" % n, "low%d_z" % n, "out%d" % n
        own = low.at[n, c * np_ + p]
        with jax.named_scope("g%d_send" % n):
            for d in far_p:
                put(pn, d // ny, own, own, plane_dev(d))
            for d in far_z:
                put(zn, 0, own, low_z.at[n, z], zdev(d, c))
            sent(pn, low.at[n, pl.ds(0, np_ - 1)])
            sent(zn, low_z.at[n, pl.ds(0, nz - 1)])
            sent(dn, low.at[n, pl.ds(0, np_)])
        with jax.named_scope("h%d_first" % n):
            first()

        def group_of(core, dx):
            return low.at[n, pl.ds(core * np_ + xs[(nx - dx) % nx] * ny, ny)]

        def own_group(dx):
            group = group_of(c, dx)
            got(pn, dx, low.at[n, pl.ds(0, ny - 1)] if dx == 0 else group)
            put(dn, dx, group, group, twin)

        def twin_group(dx):
            got(dn, dx, group_of(oc, dx))

        def times(core, dx, t):
            base = core * np_ + xs[(nx - dx) % nx] * ny
            fields = jnp.concatenate([low[n, base + q] for q in range(ny)], 1)
            row = pl.multiple_of(base * B, B * ny)
            return mm(fields, kern[t, pl.ds(row, B * ny), :])

        def add_tiles(groups, fresh):
            for t in range(half):
                out = times(*groups[0], t)
                for group in groups[1:]:
                    out = out + times(*group, t)
                for s in range(2):
                    piece = out[:, s * B:(s + 1) * B]
                    zz = 2 * t + s
                    outb[n, zz] = piece if fresh else outb[n, zz] + piece

        spans = sorted(range(nx), key=lambda d: hops(d, nx))
        with jax.named_scope("i%d_gather_a" % n):
            own_group(spans[0])
        with jax.named_scope("i%d_gather_b" % n):
            add_tiles([(c, spans[0])], True)
        with jax.named_scope("i%d_gather_c" % n):
            for dx in spans[1:]:
                own_group(dx)
            twin_group(spans[0])
        with jax.named_scope("i%d_gather_d" % n):
            add_tiles([(c, dx) for dx in spans[1:]] + [(oc, spans[0])], False)
            flush()
        with jax.named_scope("i%d_gather_e" % n):
            got(zn, 0, low_z.at[n, pl.ds(0, nz - 1)])
            for dx in spans[1:]:
                twin_group(dx)

        with jax.named_scope("j%d_tiles" % n):
            sums = None
            for t in range(half):
                out = times(oc, spans[1], t)
                for dx in spans[2:]:
                    out = out + times(oc, dx, t)
                for s in range(2):
                    zz = 2 * t + s
                    piece = blend(zz, outb[n, zz] + out[:, s * B:(s + 1) * B])
                    outb[n, zz] = piece
                    terms = each(zz, piece)
                    sums = terms if sums is None else [a + b for a, b in zip(sums, terms)]
            for d in far_z:
                put(on, 0, outb.at[n, zs[d]], rcv.at[n, z], zdev(d, c))
            sent(on, outb.at[n, pl.ds(0, nz - 1)])
        with jax.named_scope("k%d_last" % n):
            last(sums)
        with jax.named_scope("l%d_reduce" % n):
            total = outb[n, z]
            got(on, 0, rcv.at[n, pl.ds(0, nz - 1)])
            for d in near_z:
                total = total + rcv[n, zfrom(d)]
        return total

    def z_start(name, buf, value):
        buf[z] = value
        for d in far_z:
            put(name + "_z", 0, buf.at[z], buf.at[z], zdev(d, c))
        sent(name + "_z", buf.at[pl.ds(0, nz - 1)])

    def z_end(name, buf):
        got(name + "_z", 0, buf.at[pl.ds(0, nz - 1)])
        return sum_all(buf, nz)

    def p_start(name, buf, value):
        slot = c * np_ + p
        buf[slot] = value
        for d in far_p:
            put(name + "_p", 0, buf.at[slot], buf.at[slot], plane_dev(d, oc))
            put(name + "_p", 0, buf.at[slot], buf.at[slot], plane_dev(d))
        put(name + "_p", 0, buf.at[slot], buf.at[slot], twin)
        sent(name + "_p", buf.at[pl.ds(0, 2 * np_ - 1)])

    def p_end(name, buf):
        got(name + "_p", 0, buf.at[pl.ds(0, 2 * np_ - 1)])
        return sum_all(buf, 2 * np_)

    def sum_all(buf, count):
        parts = [buf[k] for k in range(count)]
        while len(parts) > 1:
            parts = [a + b for a, b in zip(parts[::2], parts[1::2])]
        return parts[0]

    def spread(row):
        return jnp.broadcast_to(row, (128, 128)).T

    def lane_sums(arrays):
        return jnp.sum(jnp.concatenate(arrays, 0).T, 0, keepdims=True)

    def first0():
        lax.fori_loop(early, np_, kern_block, 0)

    def each0(zz, piece):
        return [piece * low_z[0, zz].astype(F32)]

    def blend0(zz, piece):
        return piece

    def near_alpha(row):
        both = spread(row)
        dot, norm = jnp.maximum(both[:S], 0.0), both[S:]
        return jnp.where(norm > 0.0, norm, 1.0) / jnp.where(norm > 0.0, dot + JITTER * norm, 1.0)

    def last0(sums):
        r = rhs_s[1]
        p_start("cur0", cur_p.at[0], lane_sums([*sums, r * r]))
        row = p_end("cur0", cur_p.at[0])
        z_start("cur0", cur_z.at[0], row)
        rhs_s[4] = near_alpha(row)

    k0 = matvec(0, first0, blend0, each0, last0)
    with jax.named_scope("m_alpha"):
        rhs = rhs_s[1]
        q1 = k0 + JITTER * rhs
        rhs_s[2] = k0
        basis = rhs - rhs_s[4] * q1
        low[1, c * np_ + p] = basis.astype(BF16)
        low_z[1, z] = basis.astype(BF16)
        rhs_s[3] = q1

    def first1():
        r, k, q1 = rhs_s[1], rhs_s[2], rhs_s[3]
        sums = spread(z_end("cur0", cur_z.at[0]))
        m0 = sums[S:]
        alpha = m0 / (sums[:S] + JITTER * m0)
        new = r - alpha * q1
        rhs_s[3] = new
        rhs_s[4] = alpha
        rhs_s[5] = m0
        sums = lane_sums([new * new, new * r, new * k, r * k])
        z_start("mom", mom_z, jnp.concatenate([sums[:, :128], sums[:, 128:]], 0))
        for zz in range(nz):
            mixes[zz] = alpha / near_alpha(cur_z[0, zz])

    def blend1(zz, piece):
        mix = mixes[z]
        return mix * piece + (1.0 - mix) * outb[0, zz]

    def each1(zz, piece):
        mix, r = mixes[zz], low_z[0, zz].astype(F32)
        return [piece * (mix * low_z[1, zz].astype(F32) + (1.0 - mix) * r), piece * r]

    def last1(sums):
        p_start("cur1", cur_p.at[1], lane_sums(sums))
        p_start("mom", mom_p, z_end("mom", mom_z))
        z_start("cur1", cur_z.at[1], p_end("cur1", cur_p.at[1]))

    k1 = matvec(1, first1, blend1, each1, last1)
    with jax.named_scope("n_finish"):
        prior, r, k0, r1, alpha, m0 = (rhs_s[k] for k in range(6))
        mom = p_end("mom", mom_p)
        one, two = spread(mom[0:1]), spread(mom[1:2])
        n1, r1r, r1k, rk = one[:S], one[S:], two[:S], two[S:]
        beta = n1 / m0
        kd = k1 + beta * k0
        dire = r1 + beta * r
        dd = n1 + beta * (2.0 * r1r + beta * m0)
        known = beta * (r1k + beta * rk) + JITTER * dd
        part = spread(z_end("cur1", cur_z.at[1]))
        alpha2 = n1 / (part[:S] + beta * part[S:] + known)
        out_ref[:S] = prior + alpha * k0 + alpha2 * kd
        out_ref[S:] = r1 - alpha2 * (kd + JITTER * dire)

        flush()

        @pl.when(mine)
        def _():
            whole = halves.at[pl.ds(0, nz - 1)]
            rdma("prm_z", 0, whole, whole, twin).wait_send()


def body(sizes, points, targets, noise, omega, phase, weights):
    nx, nz, ny = sizes
    np_, half = nx * ny, nz // 2
    vmem = pl.BlockSpec(memory_space=pltpu.VMEM)
    hbm = pl.BlockSpec(memory_space=pltpu.HBM)
    block = pltpu.VMEM((2 * S, B), F32)
    both = pl.pallas_call(
        functools.partial(kernel, sizes),
        out_shape=block,
        in_specs=[hbm] * 6,
        out_specs=vmem,
        scratch_shapes=[
            pltpu.VMEM((D, B), F32),
            pltpu.VMEM((1, B), F32),
            pltpu.VMEM((S, B), F32),
            pltpu.VMEM((D, FB), F32),
            pltpu.VMEM((1, FB), F32),
            pltpu.VMEM((FB, S), F32),
            pltpu.VMEM((2, FB, 128), BF16),
            pltpu.VMEM((2, np_, 3, FB, 128), BF16),
            pltpu.VMEM((D, B), F32),
            pltpu.VMEM((2 * np_, D, B), F32),
            pltpu.VMEM((nz, D, B), F32),
            pltpu.VMEM((3, 128, 2 * B), BF16),
            pltpu.VMEM((S, 2 * B), F32),
            pltpu.VMEM((nz, 2, FB, 128), BF16),
            pltpu.VMEM((6, S, B), F32),
            pltpu.VMEM((2, 2 * np_, S, B), BF16),
            pltpu.VMEM((2, nz, S, B), BF16),
            pltpu.VMEM((half, 64, 2 * B), BF16),
            pltpu.VMEM((half, 2 * np_ * B, 2 * B), BF16),
            pltpu.VMEM((2, nz, S, B), F32),
            pltpu.VMEM((3, nz, S, B), F32),
            pltpu.VMEM((nz, 2, 128), F32),
            pltpu.VMEM((2 * np_, 2, 128), F32),
            pltpu.VMEM((2, nz, 1, 128), F32),
            pltpu.VMEM((2, 2 * np_, 1, 128), F32),
            pltpu.VMEM((nz, S, B), F32),
            pltpu.SemaphoreType.DMA((len(SENDS()),)),
            pltpu.SemaphoreType.DMA((sum(count for _, count in RECVS(nx)),)),
            pltpu.SemaphoreType.DMA((6,)),
        ],
        compiler_params=pltpu.CompilerParams(
            collective_id=0, has_side_effects=True, vmem_limit_bytes=62000000),
    )(points, targets[None, :], noise, omega, phase[None, :], weights)
    return both[:S], both[S:]


def build(mesh, sizes):
    finer = Mesh(mesh.devices.reshape(*sizes, mesh.shape["cols"]), AXES)
    in_specs = (
        P(None, COLS_ROWS),
        P(COLS_ROWS),
        P(None, COLS_ROWS),
        P(None, ROWS),
        P(ROWS),
        P(ROWS, None),
    )
    out_specs = (P(None, COLS_ROWS), P(None, COLS_ROWS))
    return jax.shard_map(
        functools.partial(body, sizes), mesh=finer, in_specs=in_specs, out_specs=out_specs,
        check_vma=False)


def solution(mesh):
    return build(mesh, (4, 8, 4))
```

```python
import functools
import math

import jax
import jax.numpy as jnp
from jax import lax
from jax.experimental import pallas as pl
from jax.experimental.pallas import tpu as pltpu
from jax.sharding import Mesh
from jax.sharding import PartitionSpec as P

AXES = ("px", "pz", "py", "cols")
ROWS = ("px", "pz", "py")
COLS_ROWS = ("cols", "px", "pz", "py")
MESH = pl.DeviceIdType.MESH
F32, BF16 = jnp.float32, jnp.bfloat16

D = 8
S = 64
B = 128
FB = 16
JITTER = 0.25
KERN_EARLY = 8
SPREAD = math.sqrt(4.0 * math.log2(math.e))
SINE = [(-1) ** k * (2.0 * math.pi) ** (2 * k + 1) / math.factorial(2 * k + 1) for k in range(6)]


def SENDS():
    table = ["prm_z", "prm0", "prm1", "pts_z", "pts_p", "pts_d", "pts_o", "prior", "mom_z", "mom_p"]
    for n in "01":
        table += ["low%s_p" % n, "low%s_d" % n, "low%s_z" % n, "out%s" % n, "cur%s_z" % n, "cur%s_p" % n]
    return table


def RECVS(nx):
    several = {"prm_z": 4}
    for name in ("low0_p", "low0_d", "low1_p", "low1_d"):
        several[name] = nx
    return [(name, several.get(name, 1)) for name in SENDS()]


def three_parts(a):
    one = a.astype(BF16).astype(F32)
    rest = a - one
    two = rest.astype(BF16).astype(F32)
    three = (rest - two).astype(BF16).astype(F32)
    return one, two, three


def rows_of(pieces, width):
    row = lax.broadcasted_iota(jnp.int32, (8, width), 0)
    out = jnp.zeros((8, width), F32)
    for k, piece in enumerate(pieces):
        out = jnp.where(row == k, piece, out)
    return out


def exponent_left(points):
    scaled = points * SPREAD
    a1, a2, a3 = three_parts(scaled)
    n1, n2, n3 = three_parts(-0.5 * jnp.sum(scaled * scaled, 0, keepdims=True))
    width = points.shape[1]
    norms = rows_of((n1, n2, n3, 1.0, 1.0, 1.0), width)
    return jnp.concatenate([a1, a1, a2, a2, a1, a3, norms, jnp.zeros((8, width), F32)], 0)


def exponent_right(points):
    scaled = points * SPREAD
    b1, b2, b3 = three_parts(scaled)
    n1, n2, n3 = three_parts(-0.5 * jnp.sum(scaled * scaled, 0, keepdims=True))
    width = points.shape[1]
    norms = rows_of((1.0, 1.0, 1.0, n1, n2, n3), width)
    return jnp.concatenate([b1, b2, b1, b2, b3, b1, norms, jnp.zeros((8, width), F32)], 0)


def cos_turns(t):
    r = t - jnp.floor(t + 0.5)
    v = 0.25 - jnp.abs(r)
    w = v * v
    acc = jnp.full_like(w, SINE[-1])
    for c in SINE[-2::-1]:
        acc = acc * w + c
    return acc * v


def mm(a, b, dims=(((1,), (0,)), ((), ()))):
    return lax.dot_general(a, b, dims, preferred_element_type=F32)


def kernel(
    sizes,
    pts_hbm, tgt_hbm, noise_hbm, omega_hbm, phase_hbm, weights_hbm,
    out_ref,
    pts, tgt, noise, omega, phase, weights,
    prm_own, bundle, ptw, ptsj, ptsi, pside, prior_s, halves, rhs_s, low, low_z, right, kern, outb, rcv,
    mom_z, mom_p, cur_z, cur_p, mixes, send, recv, local,
):
    nx, nz, ny = sizes
    np_, half = nx * ny, nz // 2
    nfeat = nx * nz * ny * FB
    x, z, y, c = (lax.axis_index(a) for a in AXES)
    xs = [x] + [lax.rem(x + d, nx) for d in range(1, nx)]
    ys = [y] + [lax.rem(y + d, ny) for d in range(1, ny)]
    zs = [z] + [lax.rem(z + d, nz) for d in range(1, nz)]
    p = x * ny + y
    oc = 1 - c
    twin = (x, z, y, oc)

    arrivals = []
    for k, (src, dst) in enumerate((
        (weights_hbm, weights), (omega_hbm, omega), (phase_hbm, phase), (pts_hbm, pts),
        (tgt_hbm, tgt), (noise_hbm, noise),
    )):
        copy = pltpu.make_async_copy(src, dst, local.at[k])
        copy.start()
        arrivals.append(copy)

    at = {}
    top = 0
    for name, count in RECVS(nx):
        at[name] = top
        top += count
    order = {name: k for k, name in enumerate(SENDS())}

    def rdma(name, k, src, dst, dev):
        return pltpu.make_async_remote_copy(
            src_ref=src, dst_ref=dst, send_sem=send.at[order[name]], recv_sem=recv.at[at[name] + k],
            device_id=dev, device_id_type=MESH)

    pending = []

    def put(name, k, src, dst, dev):
        rdma(name, k, src, dst, dev).start()

    def sent(name, whole):
        pending.append((name, whole))

    def flush():
        for name, whole in pending:
            rdma(name, 0, whole, whole, twin).wait_send()
        pending.clear()

    def got(name, k, dst):
        rdma(name, k, dst, dst, twin).wait_recv()

    def hops(d, n):
        return min(d, n - d)

    def dxy(d):
        return d // ny, d % ny

    near_p = sorted(range(1, np_), key=lambda d: hops(d // ny, nx) + hops(d % ny, ny))
    far_p = near_p[::-1]
    near_z = sorted(range(1, nz), key=lambda d: hops(d, nz))
    far_z = near_z[::-1]

    def plane_dev(d, core=c):
        dx, dy = dxy(d)
        return (xs[dx], z, ys[dy], core)

    def plane_slot(d):
        dx, dy = dxy(d)
        return xs[(nx - dx) % nx] * ny + ys[(ny - dy) % ny]

    def zdev(d, core):
        return (x, zs[d], y, core)

    def zfrom(d):
        return zs[(nz - d) % nz]

    with jax.named_scope("a_barrier"):
        bar = pltpu.get_barrier_semaphore()

        def greet(dev):
            pl.semaphore_signal(bar, inc=1, device_id=dev, device_id_type=MESH)

        for d in far_p:
            greet(plane_dev(d))
            greet(plane_dev(d, oc))
        for d in far_z:
            greet(zdev(d, c))
        greet(twin)

        turn = 1.0 / (2.0 * math.pi)
        for copy in arrivals[:4]:
            copy.wait()
        lane = lax.broadcasted_iota(jnp.int32, (FB, 128), 1)
        row = lax.broadcasted_iota(jnp.int32, (FB, 128), 0)
        angles = jnp.concatenate([omega[...], phase[...], jnp.zeros((FB - D - 1, FB), F32)], 0) * turn
        packed = jnp.zeros((FB, 128), F32)
        flip = (((0,), (0,)), ((), ()))
        for k, piece in enumerate(three_parts(angles)):
            spot = jnp.where(row < D, S + k * D + row, S + 3 * D + k)
            pick = jnp.where((lane == spot) & (row <= D), 1.0, 0.0)
            packed = packed + mm(piece.astype(BF16), pick.astype(BF16), flip)
        w1 = weights[...].astype(BF16)
        w2 = (weights[...] - w1.astype(F32)).astype(BF16)
        wide = lax.broadcasted_iota(jnp.int32, (S, 128), 1)
        deep = lax.broadcasted_iota(jnp.int32, (S, 128), 0)
        once = jnp.where(wide == deep, 1.0, 0.0).astype(BF16)
        twice = jnp.where((wide == deep) | (wide == deep + S), 1.0, 0.0).astype(BF16)
        prm_own[0] = (packed + mm(w1, once)).astype(BF16)
        prm_own[1] = mm(w2, twice).astype(BF16)
        pl.semaphore_wait(bar, 1 + (nz - 1) + 2 * (np_ - 1))

    mine = lax.rem(z, 2) == c
    zslot = lax.div(z, 2)

    with jax.named_scope("b_prm_z"):
        par = lax.rem(z + c, 2)
        turnout = {1: 0, 7: 1, 3: 2, 5: 3, 2: 1, 6: 2, 4: 3}
        places = [par, 2 + 5 * par, 6 - 3 * par, 4 + par]

        @pl.when(mine)
        def _():
            for d in far_z:
                put("prm_z", turnout[d], prm_own, halves.at[d], zdev(d, c))
            halves[0] = prm_own[...]

        put("pts_o", 0, pts, ptw, twin)
        sent("pts_o", pts)
        for d in far_p:
            put("pts_p", 0, pts, ptsj.at[c * np_ + p], plane_dev(d))
        for d in far_z:
            put("pts_z", 0, pts, ptsi.at[z], zdev(d, c))
        sent("pts_p", ptsj.at[pl.ds(0, np_ - 1)])
        sent("pts_z", ptsi.at[pl.ds(0, nz - 1)])
        ptsj[c * np_ + p] = pts[...]
        ptsi[z] = pts[...]

        left_lanes = lax.broadcasted_iota(jnp.int32, (FB, 128), 1) < S
        for stage in range(2):
            if stage == 0:
                @pl.when(jnp.logical_not(mine))
                def _():
                    got("prm_z", 0, halves.at[1])
            else:
                got("prm_z", 2, halves.at[places[2]])
            got("prm_z", 2 * stage + 1, halves.at[places[2 * stage + 1]])
            one, two = halves[places[2 * stage]], halves[places[2 * stage + 1]]
            bundle[stage, p, 0] = one[0]
            bundle[stage, p, 1] = two[0]
            bundle[stage, p, 2] = jnp.where(left_lanes, one[1].astype(F32), two[1].astype(F32)).astype(BF16)
            name = "prm%d" % stage
            for d in far_p:
                put(name, 0, bundle.at[stage, p], bundle.at[stage, p], plane_dev(d))
            sent(name, bundle.at[stage, pl.ds(0, np_ - 1)])

    with jax.named_scope("c_points"):
        got("pts_o", 0, ptw)
        got("pts_p", 0, ptsj.at[pl.ds(0, np_ - 1)])
        here = ptsj.at[pl.ds(c * np_, np_)]
        put("pts_d", 0, here, here, twin)
        sent("pts_d", here)
        got("pts_z", 0, ptsi.at[pl.ds(0, nz - 1)])
        both = jnp.concatenate([pts[...], ptw[...]], 1)
        b1, b2, b3 = three_parts(both)
        none = jnp.zeros((S, 2 * B), F32)
        ones = rows_of((1.0, 1.0, 1.0), 2 * B)
        pside[0] = jnp.concatenate([none, b1, b1, b1, ones, none[:32]], 0).astype(BF16)
        pside[1] = jnp.concatenate([none, b2, b2, none[:48]], 0).astype(BF16)
        pside[2] = jnp.concatenate([none, b3, none[:56]], 0).astype(BF16)
        for t in range(half):
            two = jnp.concatenate([ptsi[2 * t], ptsi[2 * t + 1]], 1)
            right[t] = exponent_right(two).astype(BF16)
        got("pts_d", 0, ptsj.at[pl.ds(oc * np_, np_)])

    def kern_block(j, carry):
        two = jnp.concatenate([ptsj[2 * j], ptsj[2 * j + 1]], 1)
        left = exponent_left(two).T.astype(BF16)
        row = pl.multiple_of(j * 2 * B, 2 * B)
        for t in range(half):
            kern[t, pl.ds(row, 2 * B), :] = jnp.exp2(mm(left, right[t])).astype(BF16)
        return carry

    early = (np_ * KERN_EARLY) // 16
    with jax.named_scope("d_kern"):
        lax.fori_loop(0, early, kern_block, 0)

    with jax.named_scope("e_prior"):
        spans = sorted(range(nx), key=lambda d: hops(d, nx))
        for stage in range(2):
            columns = []

            def columns_in(some):
                for dx in some:
                    base = xs[(nx - dx) % nx] * ny
                    columns.append(base)

            got("prm%d" % stage, 0, bundle.at[stage, pl.ds(0, np_ - 1)])
            columns_in(spans)

            def features(bases, lanes):
                pick = [(base + q, k) for k in range(2) for base in bases for q in range(ny)]
                part = jnp.concatenate([bundle[stage, slot, k] for slot, k in pick], 0)
                rest = jnp.concatenate([bundle[stage, base + q, 2] for base in bases for q in range(ny)], 0)
                cut = rest.shape[0]
                turns = mm(part, pside[0, :, lanes]) + mm(part, pside[1, :, lanes]) + mm(part, pside[2, :, lanes])
                feats = cos_turns(turns)
                f1 = feats.astype(BF16)
                f2 = (feats - f1.astype(F32)).astype(BF16)
                total = (mm(part, f1, flip) + mm(part, f2, flip))[:S]
                return total + mm(rest, f1[:cut], flip)[:S] + mm(rest, f1[cut:], flip)[S:]

            couples = (columns[:2], columns[2:])
            if stage == 0:
                prior_s[...] = sum(features(bases, slice(0, 2 * B)) for bases in couples)
            else:
                rcv[2, 1] = prior_s[:, B:] + sum(features(bases, slice(B, 2 * B)) for bases in couples)
                put("prior", 0, rcv.at[2, 1], rcv.at[2, 0], twin)
                sent("prior", rcv.at[2, 1])
                prior_own = prior_s[:, :B] + sum(features(bases, slice(0, B)) for bases in couples)

    with jax.named_scope("f_swap"):
        for copy in arrivals[4:]:
            copy.wait()
        got("prior", 0, rcv.at[2, 0])
        scale = math.sqrt(2.0 / nfeat)
        prior = scale * (prior_own + rcv[2, 0])
        rhs = tgt[...] - prior - 0.5 * noise[...]
        rhs_s[0] = prior
        rhs_s[1] = rhs
        low[0, c * np_ + p] = rhs.astype(BF16)
        low_z[0, z] = rhs.astype(BF16)

    def matvec(n, first, blend, each, last):
        pn, dn, zn, on = "low%d_p" % n, "low%d_d" % n, "low%d_z" % n, "out%d" % n
        own = low.at[n, c * np_ + p]
        with jax.named_scope("g%d_send" % n):
            for d in far_p:
                put(pn, d // ny, own, own, plane_dev(d))
            for d in far_z:
                put(zn, 0, own, low_z.at[n, z], zdev(d, c))
            sent(pn, low.at[n, pl.ds(0, np_ - 1)])
            sent(zn, low_z.at[n, pl.ds(0, nz - 1)])
            sent(dn, low.at[n, pl.ds(0, np_)])
        with jax.named_scope("h%d_first" % n):
            first()

        def group_of(core, dx):
            return low.at[n, pl.ds(core * np_ + xs[(nx - dx) % nx] * ny, ny)]

        def own_group(dx):
            group = group_of(c, dx)
            got(pn, dx, low.at[n, pl.ds(0, ny - 1)] if dx == 0 else group)
            put(dn, dx, group, group, twin)

        def twin_group(dx):
            got(dn, dx, group_of(oc, dx))

        def times(core, dx, t):
            base = core * np_ + xs[(nx - dx) % nx] * ny
            fields = jnp.concatenate([low[n, base + q] for q in range(ny)], 1)
            row = pl.multiple_of(base * B, B * ny)
            return mm(fields, kern[t, pl.ds(row, B * ny), :])

        def add_tiles(groups, fresh):
            for t in range(half):
                out = times(*groups[0], t)
                for group in groups[1:]:
                    out = out + times(*group, t)
                for s in range(2):
                    piece = out[:, s * B:(s + 1) * B]
                    zz = 2 * t + s
                    outb[n, zz] = piece if fresh else outb[n, zz] + piece

        spans = sorted(range(nx), key=lambda d: hops(d, nx))
        with jax.named_scope("i%d_gather_a" % n):
            own_group(spans[0])
        with jax.named_scope("i%d_gather_b" % n):
            add_tiles([(c, spans[0])], True)
        with jax.named_scope("i%d_gather_c" % n):
            for dx in spans[1:]:
                own_group(dx)
            twin_group(spans[0])
        with jax.named_scope("i%d_gather_d" % n):
            add_tiles([(c, dx) for dx in spans[1:]] + [(oc, spans[0])], False)
            flush()
        with jax.named_scope("i%d_gather_e" % n):
            got(zn, 0, low_z.at[n, pl.ds(0, nz - 1)])
            for dx in spans[1:]:
                twin_group(dx)

        with jax.named_scope("j%d_tiles" % n):
            sums = None
            for t in range(half):
                out = times(oc, spans[1], t)
                for dx in spans[2:]:
                    out = out + times(oc, dx, t)
                for s in range(2):
                    zz = 2 * t + s
                    piece = blend(zz, outb[n, zz] + out[:, s * B:(s + 1) * B])
                    outb[n, zz] = piece
                    terms = each(zz, piece)
                    sums = terms if sums is None else [a + b for a, b in zip(sums, terms)]
            for d in far_z:
                put(on, 0, outb.at[n, zs[d]], rcv.at[n, z], zdev(d, c))
            sent(on, outb.at[n, pl.ds(0, nz - 1)])
        with jax.named_scope("k%d_last" % n):
            last(sums)
        with jax.named_scope("l%d_reduce" % n):
            total = outb[n, z]
            got(on, 0, rcv.at[n, pl.ds(0, nz - 1)])
            for d in near_z:
                total = total + rcv[n, zfrom(d)]
        return total

    def z_start(name, buf, value):
        buf[z] = value
        for d in far_z:
            put(name + "_z", 0, buf.at[z], buf.at[z], zdev(d, c))
        sent(name + "_z", buf.at[pl.ds(0, nz - 1)])

    def z_end(name, buf):
        got(name + "_z", 0, buf.at[pl.ds(0, nz - 1)])
        return sum_all(buf, nz)

    def p_start(name, buf, value):
        slot = c * np_ + p
        buf[slot] = value
        for d in far_p:
            put(name + "_p", 0, buf.at[slot], buf.at[slot], plane_dev(d, oc))
            put(name + "_p", 0, buf.at[slot], buf.at[slot], plane_dev(d))
        put(name + "_p", 0, buf.at[slot], buf.at[slot], twin)
        sent(name + "_p", buf.at[pl.ds(0, 2 * np_ - 1)])

    def p_end(name, buf):
        got(name + "_p", 0, buf.at[pl.ds(0, 2 * np_ - 1)])
        return sum_all(buf, 2 * np_)

    def sum_all(buf, count):
        parts = [buf[k] for k in range(count)]
        while len(parts) > 1:
            parts = [a + b for a, b in zip(parts[::2], parts[1::2])]
        return parts[0]

    def spread(row):
        return jnp.broadcast_to(row, (128, 128)).T

    def lane_sums(arrays):
        return jnp.sum(jnp.concatenate(arrays, 0).T, 0, keepdims=True)

    def first0():
        lax.fori_loop(early, np_, kern_block, 0)

    def each0(zz, piece):
        return [piece * low_z[0, zz].astype(F32)]

    def blend0(zz, piece):
        return piece

    def near_alpha(row):
        both = spread(row)
        dot, norm = jnp.maximum(both[:S], 0.0), both[S:]
        return jnp.where(norm > 0.0, norm, 1.0) / jnp.where(norm > 0.0, dot + JITTER * norm, 1.0)

    def last0(sums):
        r = rhs_s[1]
        p_start("cur0", cur_p.at[0], lane_sums([*sums, r * r]))
        row = p_end("cur0", cur_p.at[0])
        z_start("cur0", cur_z.at[0], row)
        rhs_s[4] = near_alpha(row)

    k0 = matvec(0, first0, blend0, each0, last0)
    with jax.named_scope("m_alpha"):
        rhs = rhs_s[1]
        q1 = k0 + JITTER * rhs
        rhs_s[2] = k0
        basis = rhs - rhs_s[4] * q1
        low[1, c * np_ + p] = basis.astype(BF16)
        low_z[1, z] = basis.astype(BF16)
        rhs_s[3] = q1

    def first1():
        r, k, q1 = rhs_s[1], rhs_s[2], rhs_s[3]
        sums = spread(z_end("cur0", cur_z.at[0]))
        m0 = sums[S:]
        alpha = m0 / (sums[:S] + JITTER * m0)
        new = r - alpha * q1
        rhs_s[3] = new
        rhs_s[4] = alpha
        rhs_s[5] = m0
        sums = lane_sums([new * new, new * r, new * k, r * k])
        z_start("mom", mom_z, jnp.concatenate([sums[:, :128], sums[:, 128:]], 0))
        for zz in range(nz):
            mixes[zz] = alpha / near_alpha(cur_z[0, zz])

    def blend1(zz, piece):
        mix = mixes[z]
        return mix * piece + (1.0 - mix) * outb[0, zz]

    def each1(zz, piece):
        mix, r = mixes[zz], low_z[0, zz].astype(F32)
        return [piece * (mix * low_z[1, zz].astype(F32) + (1.0 - mix) * r), piece * r]

    def last1(sums):
        p_start("cur1", cur_p.at[1], lane_sums(sums))
        p_start("mom", mom_p, z_end("mom", mom_z))
        z_start("cur1", cur_z.at[1], p_end("cur1", cur_p.at[1]))

    k1 = matvec(1, first1, blend1, each1, last1)
    with jax.named_scope("n_finish"):
        prior, r, k0, r1, alpha, m0 = (rhs_s[k] for k in range(6))
        mom = p_end("mom", mom_p)
        one, two = spread(mom[0:1]), spread(mom[1:2])
        n1, r1r, r1k, rk = one[:S], one[S:], two[:S], two[S:]
        beta = n1 / m0
        kd = k1 + beta * k0
        dire = r1 + beta * r
        dd = n1 + beta * (2.0 * r1r + beta * m0)
        known = beta * (r1k + beta * rk) + JITTER * dd
        part = spread(z_end("cur1", cur_z.at[1]))
        alpha2 = n1 / (part[:S] + beta * part[S:] + known)
        out_ref[:S] = prior + alpha * k0 + alpha2 * kd
        out_ref[S:] = r1 - alpha2 * (kd + JITTER * dire)

        flush()

        @pl.when(mine)
        def _():
            whole = halves.at[pl.ds(0, nz - 1)]
            rdma("prm_z", 0, whole, whole, twin).wait_send()


def body(sizes, points, targets, noise, omega, phase, weights):
    nx, nz, ny = sizes
    np_, half = nx * ny, nz // 2
    vmem = pl.BlockSpec(memory_space=pltpu.VMEM)
    hbm = pl.BlockSpec(memory_space=pltpu.HBM)
    block = pltpu.VMEM((2 * S, B), F32)
    both = pl.pallas_call(
        functools.partial(kernel, sizes),
        out_shape=block,
        in_specs=[hbm] * 6,
        out_specs=vmem,
        scratch_shapes=[
            pltpu.VMEM((D, B), F32),
            pltpu.VMEM((1, B), F32),
            pltpu.VMEM((S, B), F32),
            pltpu.VMEM((D, FB), F32),
            pltpu.VMEM((1, FB), F32),
            pltpu.VMEM((FB, S), F32),
            pltpu.VMEM((2, FB, 128), BF16),
            pltpu.VMEM((2, np_, 3, FB, 128), BF16),
            pltpu.VMEM((D, B), F32),
            pltpu.VMEM((2 * np_, D, B), F32),
            pltpu.VMEM((nz, D, B), F32),
            pltpu.VMEM((3, 128, 2 * B), BF16),
            pltpu.VMEM((S, 2 * B), F32),
            pltpu.VMEM((nz, 2, FB, 128), BF16),
            pltpu.VMEM((6, S, B), F32),
            pltpu.VMEM((2, 2 * np_, S, B), BF16),
            pltpu.VMEM((2, nz, S, B), BF16),
            pltpu.VMEM((half, 64, 2 * B), BF16),
            pltpu.VMEM((half, 2 * np_ * B, 2 * B), BF16),
            pltpu.VMEM((2, nz, S, B), F32),
            pltpu.VMEM((3, nz, S, B), F32),
            pltpu.VMEM((nz, 2, 128), F32),
            pltpu.VMEM((2 * np_, 2, 128), F32),
            pltpu.VMEM((2, nz, 1, 128), F32),
            pltpu.VMEM((2, 2 * np_, 1, 128), F32),
            pltpu.VMEM((nz, S, B), F32),
            pltpu.SemaphoreType.DMA((len(SENDS()),)),
            pltpu.SemaphoreType.DMA((sum(count for _, count in RECVS(nx)),)),
            pltpu.SemaphoreType.DMA((6,)),
        ],
        compiler_params=pltpu.CompilerParams(
            collective_id=0, has_side_effects=True, vmem_limit_bytes=62000000),
    )(points, targets[None, :], noise, omega, phase[None, :], weights)
    return both[:S], both[S:]


def build(mesh, sizes):
    finer = Mesh(mesh.devices.reshape(*sizes, mesh.shape["cols"]), AXES)
    in_specs = (
        P(None, COLS_ROWS),
        P(COLS_ROWS),
        P(None, COLS_ROWS),
        P(None, ROWS),
        P(ROWS),
        P(ROWS, None),
    )
    out_specs = (P(None, COLS_ROWS), P(None, COLS_ROWS))
    return jax.shard_map(
        functools.partial(body, sizes), mesh=finer, in_specs=in_specs, out_specs=out_specs,
        check_vma=False)


def solution(mesh):
    return build(mesh, (4, 8, 4))
```
